256 devices in a mesh: fac: 32 (over y, z), cust: 8 (over x, core).
Axes of the slice: x: 4, y: 4, z: 8, core: 2. Of those that a mesh axis runs over, the one named last changes fastest.
Arguments:
- fac_coords: bfloat16 [16384, 128], P('fac'), may hold values from -6 to 6
- cust_coords: bfloat16 [131072, 128], P(('cust', 'fac')), may hold values from -6 to 6
- open_flags: int32 [16384], P('fac'), may hold values 0 or 1
- demand: int32 [131072], P('cust'), may hold values from 1 to 4
- fixed_cost: float32 [16384], P('fac'), may hold values from 0 to 64
- capacity: float32 [16384], P('fac'), may hold values from 16 to 64
- cap_mult: float32 [16384], P('fac'), may hold values from 0 to 0.1
- cover_mult: float32 [131072], P('cust'), may hold values from 0 to 2, as said below
Outputs:
- cover_final: float32 [131072], P('cust')
- cap_final: float32 [16384], P('fac')
- bounds: float32 [3], replicated
The draws below stay inside these ranges and needn't reach their ends.
Inputs may be any that keep to these rules, and one draw needn't show every extreme that they name: `cover_mult`: initial coverage multipliers, all in one band of width 0.4.
All inputs are finite; a program needn't handle non-finite values. No bound on the sum of `open_flags` on one device may be relied on, other than what follows from the above.
Results may differ from the reference program's by a relative error of at most 0.0003.
Values may be sent and summed in bfloat16 or wider, within the bound.
A program may use at most 64 MiB of HBM per device.

```python
import math
import jax
import jax.numpy as jnp
from jax import lax

K = 128
ITERS = 3
F = 16384
C = 131072


def draw_cover_mult(key, part):
    tau = 0.1
    level = 2.125 - tau * (math.log(F / 2.0) + 300.0 / K)
    spread = jax.random.uniform(key, (C,), jnp.float32, -0.2, 0.2)
    return (level + spread).astype(jnp.float32)


def with_ends(array, rng, smallest, top_value):
    index_at = [jax.random.randint(jax.random.fold_in(rng, axis), (), 0, length) for axis, length in enumerate(array.shape)]
    longest = array.shape.index(max(array.shape))
    neighbour = index_at[:longest] + [(index_at[longest] + 1) % array.shape[longest]] + index_at[longest + 1:]
    return array.at[tuple(index_at)].set(smallest).at[tuple(neighbour)].set(top_value)


def levels(own_key, dims, split, low, high):
    def one(dim, blocks):
        heights = jax.random.uniform(jax.random.fold_in(jax.random.fold_in(own_key, 6), dim), (blocks,), jnp.float32, low / len(split), high / len(split))
        return jnp.repeat(jnp.exp(heights), dims[dim] // blocks).reshape((-1,) + (1,) * (len(dims) - dim - 1))

    loudness = one(*split[0])
    for cut in split[1:]:
        loudness = loudness * one(*cut)
    return loudness


def noise(stream_key, shape, scale, reach, pieces=(), kind=jnp.bfloat16):
    gain = levels(stream_key, shape, pieces, -0.22, 0.18) if pieces else 1.0
    entries = jax.random.normal(stream_key, shape, jnp.float32) * scale * gain
    return jnp.minimum(jnp.maximum(entries, -reach), reach).astype(kind)


def setup_inputs(seed: int = 0) -> dict:
    key_of = jax.random.split(jax.random.key(seed), 9)
    return {
        "fac_coords": noise(key_of[0], (F, K), 1.0, 6.0, ((0, 32),)),
        "cust_coords": noise(key_of[1], (C, K), 1.0, 6.0, ((0, 256),)),
        "open_flags": with_ends((jax.random.randint(key_of[2], (F,), 0, 2) < 1).astype(jnp.int32), jax.random.fold_in(key_of[2], 1), 0, 1),
        "demand": with_ends(jax.random.randint(key_of[3], (C,), 1, 5), jax.random.fold_in(key_of[3], 1), 1, 4).astype(jnp.int32),
        "fixed_cost": jnp.clip(64.0 * jax.random.uniform(key_of[4], (F,), jnp.float32) ** levels(key_of[4], (F,), ((0, 32),), -0.2, 0.2), 0.0, 64.0),
        "capacity": jnp.clip(16.0 + 48.0 * jax.random.uniform(key_of[5], (F,), jnp.float32) ** levels(key_of[5], (F,), ((0, 32),), -0.2, 0.2), 16.0, 64.0),
        "cap_mult": jnp.clip(0.1 * jax.random.uniform(key_of[6], (F,), jnp.float32) ** levels(key_of[6], (F,), ((0, 32),), -0.2, 0.2), 0.0, 0.1),
        "cover_mult": draw_cover_mult(jax.random.fold_in(key_of[8], 71), 0),
    }


def reference(fac_coords, cust_coords, open_flags, demand, fixed_cost, capacity, cap_mult, cover_mult):
    tau = 0.1
    fac_block = 256
    n_fac = fac_coords.shape[0]
    n_cust = cust_coords.shape[0]
    width = fac_coords.shape[1]
    fac_block = min(fac_block, n_fac)
    opened = open_flags.astype(jnp.float32)
    weight = demand.astype(jnp.float32)
    pnorm = jnp.sum(fac_coords.astype(jnp.float32) ** 2, axis=1)
    qnorm = jnp.sum(cust_coords.astype(jnp.float32) ** 2, axis=1)
    blocks = n_fac // fac_block
    lam = cover_mult
    mu = cap_mult
    bound_list = []
    for step in range(ITERS):
        size = 0.1 / (step + 1)

        def one_block(cover, index):
            start = (index * fac_block).astype(jnp.int32)
            rows = lax.dynamic_slice_in_dim(fac_coords, start, fac_block, 0)
            pn = lax.dynamic_slice_in_dim(pnorm, start, fac_block, 0)
            mu_b = lax.dynamic_slice_in_dim(mu, start, fac_block, 0)
            op_b = lax.dynamic_slice_in_dim(opened, start, fac_block, 0)
            dots = lax.dot_general(rows, cust_coords, (((1,), (1,)), ((), ())), preferred_element_type=jnp.float32)
            cost = (pn[:, None] + qnorm[None, :] - 2.0 * dots) / width
            zval = (lam[None, :] - cost - mu_b[:, None] * weight[None, :]) / tau
            share = op_b[:, None] * jax.nn.sigmoid(zval)
            load_b = jnp.sum(share * weight[None, :], axis=1)
            soft_b = -tau * op_b * jnp.sum(jax.nn.softplus(zval) * weight[None, :], axis=1)
            return cover + jnp.sum(share, axis=0), (load_b, soft_b)

        cover, pair = lax.scan(one_block, jnp.zeros((n_cust,), jnp.float32), jnp.arange(blocks, dtype=jnp.int32))
        load = pair[0].reshape(n_fac)
        soft = pair[1].reshape(n_fac)
        bound = (jnp.sum(weight * lam) + jnp.sum(opened * fixed_cost - mu * capacity + soft)) / n_cust
        bound_list.append(bound)
        lam = lam + size * weight * (1.0 - cover) / (1.0 + cover)
        mu = jnp.maximum(0.0, mu + size * (load - capacity) / (load + capacity))
    return lam, mu, jnp.stack(bound_list).astype(jnp.float32)
```

```python
import functools
import math

import jax
import jax.numpy as jnp
from jax import lax
from jax.experimental import pallas as pl
from jax.experimental.pallas import tpu as pltpu
from jax.sharding import PartitionSpec as P

MESH = pl.DeviceIdType.MESH
ITERS = 3
TAU = 0.1
ALIGN = 16
ROWS = 128
BLOCK = 512
CHUNKS = 4
NZ = 8
F32 = jnp.float32
BF16 = jnp.bfloat16
VMEM = pl.BlockSpec(memory_space=pltpu.VMEM)
SMEM = pl.BlockSpec(memory_space=pltpu.SMEM)


def split3(v):
    a = v.astype(BF16)
    r = v - a.astype(F32)
    b = r.astype(BF16)
    c = (r - b.astype(F32)).astype(BF16)
    return a, b, c


def onehot_of(open_row):
    n = open_row.shape[1]
    flags = jnp.broadcast_to(open_row.astype(F32), (16, n)).astype(BF16)
    tri = (lax.broadcasted_iota(jnp.int32, (n, n), 0) <= lax.broadcasted_iota(jnp.int32, (n, n), 1)).astype(F32).astype(BF16)
    pos = jnp.dot(flags, tri, preferred_element_type=F32)[0:1]
    pos = jnp.where(open_row > 0, pos - 1.0, -1.0).astype(jnp.int32)
    hit = lax.broadcasted_iota(jnp.int32, (n, n), 0) == pos
    return jnp.where(hit, 1.0, 0.0).astype(BF16)


def nt(a, b):
    return lax.dot_general(a, b, (((1,), (1,)), ((), ())), preferred_element_type=F32)


def tn(a, b):
    return lax.dot_general(a, b, (((0,), (0,)), ((), ())), preferred_element_type=F32)


def spots():
    f, c = lax.axis_index("fac"), lax.axis_index("cust")
    return f // NZ, lax.rem(f, NZ), c


def pre_kernel(open_ref, fac_ref, cap_ref, mu_ref, fixed_ref, demand_ref, cover_ref,
               comp_ref, info_ref, wt_ref, lam_ref, ext_ref, shut_ref):
    n, width = fac_ref.shape
    nz, cols = wt_ref.shape
    y, z, c = spots()
    for r in range(nz):
        mine = pl.ds(pl.multiple_of((y * nz + r) * cols, cols), cols)
        wt_ref[r:r + 1, :] = demand_ref[:, mine].astype(F32)
        lam_ref[r:r + 1, :] = cover_ref[:, mine]
    opened = open_ref[...].astype(F32)
    shut = mu_ref[...]
    ext = jnp.zeros((8, 128), F32)
    lane = lax.broadcasted_iota(jnp.int32, (8, 128), 1)
    sub = lax.broadcasted_iota(jnp.int32, (8, 128), 0)
    for k in range(ITERS):
        fixed = jnp.sum(opened * fixed_ref[...] - (1.0 - opened) * shut * cap_ref[...])
        ext = ext + jnp.where((lane == k) & (sub == 0) & (c == 0), fixed, 0.0)
        shut = jnp.maximum(0.0, shut - 0.1 / (k + 1))
    ext_ref[...] = ext
    shut_ref[...] = shut
    hot = onehot_of(open_ref[...])
    fac = fac_ref[...]
    comp_ref[...] = jnp.dot(hot, fac, preferred_element_type=F32).astype(BF16)
    sq = fac.astype(F32) ** 2
    s1, s2, _ = split3(sq)
    ones = jnp.ones((16, width), BF16)
    half = -0.5 * (nt(ones, s1) + nt(ones, s2))[0:1]
    rows = [jnp.ones((1, n), BF16)]
    for v in (half, mu_ref[...], cap_ref[...]):
        rows.extend(split3(v))
    rows = [r.astype(F32) for r in rows] + [jnp.zeros((6, n), F32)]
    got = nt(jnp.concatenate(rows, axis=0).astype(BF16), hot)
    rows = [got[0:1]] + [got[3 * m + 1:3 * m + 2] + got[3 * m + 2:3 * m + 3] + got[3 * m + 3:3 * m + 4] for m in range(3)]
    info_ref[...] = jnp.concatenate(rows + [jnp.zeros((4, n), F32)], axis=0)


def sync(peers):
    barrier = pltpu.get_barrier_semaphore()
    for peer in peers:
        pl.semaphore_signal(barrier, inc=1, device_id=peer, device_id_type=MESH)
    pl.semaphore_wait(barrier, len(peers))


def remote(src, dst, send, recv, peer):
    cpy = pltpu.make_async_remote_copy(src, dst, send, recv, device_id=peer, device_id_type=MESH)
    cpy.start()
    return cpy


def gather_kernel(ny, cust_ref, comp_ref, info_ref, all_ref, facs_ref, infos_ref, sz, rz, sy, ry):
    y, z, c = spots()
    hops = NZ // 2
    zp = [(y * NZ + lax.rem(z + s, NZ), c) for s in (1, NZ - 1)]
    yp = [(lax.rem(y + d, ny) * NZ + z, c) for d in range(1, ny)]
    part = cust_ref.shape[0] // CHUNKS
    sync(zp + yp)

    def move(d, s, j):
        src = lax.rem(z + (NZ - s if d == 0 else s), NZ)
        at = pl.ds(j * part, part)
        a = cust_ref.at[at] if s == 0 else all_ref.at[src, at]
        return remote(a, all_ref.at[src, at], sz.at[d, s, j], rz.at[d, s, j], zp[d])

    def valid(d, s, j):
        return s < hops - 1 or (s == hops - 1 and (j < CHUNKS // 2) == (d == 0))

    ring = {}
    for j in range(CHUNKS):
        for d in range(2):
            if valid(d, 0, j):
                ring[d, 0, j] = move(d, 0, j)
    side = []
    for k, peer in enumerate(yp):
        side.append(remote(info_ref, infos_ref.at[y], sy.at[k, 0], ry.at[k, 0], peer))
        side.append(remote(comp_ref, facs_ref.at[y], sy.at[k, 1], ry.at[k, 1], peer))
    all_ref[z] = cust_ref[...]
    facs_ref[y] = comp_ref[...]
    infos_ref[y] = info_ref[...]
    for s in range(hops):
        for j in range(CHUNKS):
            for d in range(2):
                if valid(d, s, j):
                    ring[d, s, j].wait_recv()
                    if valid(d, s + 1, j):
                        ring[d, s + 1, j] = move(d, s + 1, j)
    for cpy in ring.values():
        cpy.wait_send()
    for cpy in side:
        cpy.wait()


def step_kernel(step, ny, refs):
    first = step == 0
    if first:
        (facs_ref, infos_ref, cust_ref, lam_ref, wt_ref, ext_ref,
         load_ref, cover_ref, tot_ref, mu_out_ref, coords_ref, turned_ref, hq_ref,
         a_ref, w_ref, y_ref, x_ref, d_ref, acc_ref, cov_ref, soft_ref) = refs
    else:
        (coords_ref, infos_ref, turned_ref, hq_ref, mu_ref, lam_ref, wt_ref, ext_ref,
         load_ref, cover_ref, tot_ref,
         a_ref, w_ref, y_ref, x_ref, d_ref, acc_ref, cov_ref, soft_ref) = refs
    n = infos_ref.shape[2]
    nz, cols = lam_ref.shape
    width = coords_ref.shape[1]
    total = nz * cols
    tiles = total // BLOCK
    me_y, me_z, c = spots()
    if first:
        eye = (lax.broadcasted_iota(jnp.int32, (width, width), 0) == lax.broadcasted_iota(jnp.int32, (width, width), 1)).astype(F32).astype(BF16)
        for r in range(nz):
            turned = nt(eye, cust_ref[r])
            w_ref[0:width, r * cols:(r + 1) * cols] = turned.astype(BF16)
            turned_ref[:, r * cols:(r + 1) * cols] = turned.astype(BF16)
            hq_ref[r:r + 1, :] = 0.5 * jnp.sum(turned * turned, axis=0, keepdims=True)
    else:
        w_ref[0:width, :] = turned_ref[...]
    wt = wt_ref[...]
    lam = lam_ref[...]
    a1, a2, a3 = split3(64.0 * lam - hq_ref[...])
    one_c = jnp.ones((3, cols), F32)
    top = (lax.broadcasted_iota(jnp.int32, (16, 128), 0) == 0).astype(F32).astype(BF16)
    for r in range(nz):
        row = slice(r, r + 1)
        at = slice(r * cols, (r + 1) * cols)
        mw = jnp.broadcast_to(-64.0 * wt[row], (3, cols))
        aug = jnp.concatenate([a1[row].astype(F32), a2[row].astype(F32), a3[row].astype(F32), one_c, mw, jnp.zeros((7, cols), F32)], axis=0)
        w_ref[width:width + 16, at] = aug.astype(BF16)
        wrows = jnp.concatenate([wt[row], jnp.zeros((15, cols), F32)], axis=0).astype(BF16)
        d_ref[at, :] = tn(wrows, top).astype(BF16)
    w_ref[width + 16:, :] = jnp.zeros((width - 16, total), BF16)
    cov_ref[...] = jnp.zeros_like(cov_ref)
    soft_ref[...] = jnp.zeros_like(soft_ref)
    lane = lax.broadcasted_iota(jnp.int32, (ROWS, width), 1)
    pad = jnp.where(lane == 3, -30000.0, 0.0).astype(BF16)
    sel = (lax.broadcasted_iota(jnp.int32, (16, width), 0) == lax.broadcasted_iota(jnp.int32, (16, width), 1)).astype(F32).astype(BF16)
    offs = []
    off = jnp.int32(0)
    one_r = jnp.ones((3, n), F32)
    if not first:
        a_ref[:, 0:width] = coords_ref[...]
    for s in range(ny):
        valid = infos_ref[s, 0:1, :]
        if first:
            mu = infos_ref[s, 2:3, :] * valid
            mu_out_ref[s:s + 1, :] = mu
        else:
            mu = mu_ref[s:s + 1, :]
        b = jnp.where(valid > 0, infos_ref[s, 1:2, :], -30000.0)
        parts = [p.astype(F32) for p in split3(b) + split3(mu)]
        rows = jnp.concatenate([one_r] + parts + [jnp.zeros((7, n), F32)], axis=0).astype(BF16)
        side = tn(rows, sel).astype(BF16)
        count = jnp.sum(valid).astype(jnp.int32)
        off = pl.multiple_of(off, ALIGN)
        offs.append(off)
        if first:
            a_ref[pl.ds(off, n), 0:width] = facs_ref[s]
        a_ref[pl.ds(off, n), width:2 * width] = side
        off = off + ((count + ALIGN - 1) // ALIGN) * ALIGN
    tail = pl.multiple_of(off, ALIGN)
    if first:
        a_ref[pl.ds(tail, ROWS), 0:width] = jnp.zeros((ROWS, width), BF16)
    a_ref[pl.ds(tail, ROWS), width:2 * width] = pad
    if first:
        coords_ref[...] = a_ref[:, 0:width]
    n_blocks = (off + ROWS - 1) // ROWS
    scale = math.log2(math.e) / 6.4
    half = tiles // 2

    def dot(base, t, slot):
        y_ref[slot] = jnp.dot(a_ref[pl.ds(base, ROWS), :], w_ref[:, t * BLOCK:(t + 1) * BLOCK], preferred_element_type=F32)

    def weigh(h):
        return jnp.dot(x_ref[h], d_ref[h * half * BLOCK:(h + 1) * half * BLOCK, :], preferred_element_type=F32)

    def body(i, _):
        base = pl.multiple_of(i * ROWS, ROWS)
        acc_ref[pl.ds(base, ROWS), :] = acc_ref[pl.ds(base, ROWS), :] + weigh(1)
        for t in range(tiles):
            if t + 1 < tiles:
                dot(base, t + 1, (t + 1) % 2)
            else:
                dot(pl.multiple_of(base + ROWS, ROWS), 0, (t + 1) % 2)
            for q in range(BLOCK // 128):
                at = slice(t * BLOCK + q * 128, t * BLOCK + (q + 1) * 128)
                xat = slice((t % half) * BLOCK + q * 128, (t % half) * BLOCK + (q + 1) * 128)
                cov = cov_ref[:, at]
                soft = soft_ref[:, at]
                for r in range(0, ROWS, 64):
                    es = [jnp.exp2(y_ref[t % 2, r + 16 * s:r + 16 * s + 16, q * 128:(q + 1) * 128] * scale) for s in range(4)]
                    us = [1.0 + e for e in es]
                    p01 = us[0] * us[1]
                    p23 = us[2] * us[3]
                    r01 = 1.0 / p01
                    r23 = 1.0 / p23
                    xs = [es[0] * (us[1] * r01), es[1] * (us[0] * r01), es[2] * (us[3] * r23), es[3] * (us[2] * r23)]
                    for s in range(4):
                        x_ref[t // half, r + 16 * s:r + 16 * s + 16, xat] = xs[s].astype(BF16)
                    tot = (xs[0] + xs[1]) + (xs[2] + xs[3])
                    lg = jnp.log(p01 * p23)
                    cov = cov + (tot[0:8] + tot[8:16])
                    soft = soft + (lg[0:8] + lg[8:16])
                cov_ref[:, at] = cov
                soft_ref[:, at] = soft
            if t == half - 1:
                acc_ref[pl.ds(pl.multiple_of(base + ROWS, ROWS), ROWS), :] = weigh(0)
        return 0

    dot(0, 0, 0)
    x_ref[1] = jnp.zeros(x_ref.shape[1:], BF16)
    acc_ref[0:ROWS, :] = jnp.zeros((ROWS, 128), F32)
    lax.fori_loop(0, n_blocks, body, 0)
    end = pl.ds(pl.multiple_of(n_blocks * ROWS, ROWS), ROWS)
    acc_ref[end, :] = acc_ref[end, :] + weigh(1)
    diag = lax.broadcasted_iota(jnp.int32, (128, 128), 0) == lax.broadcasted_iota(jnp.int32, (128, 128), 1)
    for s in range(ny):
        for b in range(n // 128):
            at = pl.ds(pl.multiple_of(offs[s] + (b * 128 + ROWS), ALIGN), 128)
            got = jnp.sum(jnp.where(diag, acc_ref[at, :], 0.0), axis=0, keepdims=True)
            load_ref[s:s + 1, b * 128:(b + 1) * 128] = jnp.where(infos_ref[s, 0:1, b * 128:(b + 1) * 128] > 0, got, 0.0)
    soft = 0.0
    for r in range(nz):
        at = slice(r * cols, (r + 1) * cols)
        cover_ref[r:r + 1, :] = jnp.sum(cov_ref[:, at], axis=0, keepdims=True)
        soft = soft + soft_ref[:, at] * wt[r:r + 1]
    mu_all = mu_out_ref if first else mu_ref
    caps = infos_ref[me_y, 3:4, :]
    mine = jnp.sum(mu_all[pl.ds(me_y, 1), :] * caps)
    owned = jnp.sum(lam_ref[pl.ds(me_z, 1), :] * wt_ref[pl.ds(me_z, 1), :])
    here = owned - TAU * jnp.sum(soft) - jnp.where(c == 0, mine, 0.0)
    spot = (lax.broadcasted_iota(jnp.int32, (8, 128), 1) == step) & (lax.broadcasted_iota(jnp.int32, (8, 128), 0) == 0)
    tot_ref[...] = ext_ref[...] + jnp.where(spot, here, 0.0)


def reduce_kernel(step, ny, nc, refs):
    last = step == ITERS - 1
    if last:
        (load_ref, cover_ref, lam_ref, wt_ref, mu_ref, infos_ref, tot_ref,
         lam_out_ref, mu_out_ref, tot_out_ref,
         gotz, gotc, goty, mid, sz, rz, sc, rc, sy, ry, gott, gotp, midt, own, st, rt, sp, rp, sl, rl) = refs
    else:
        (load_ref, cover_ref, lam_ref, wt_ref, mu_ref, infos_ref,
         lam_out_ref, mu_out_ref,
         gotz, gotc, goty, mid, sz, rz, sc, rc, sy, ry) = refs
    size = 0.1 / (step + 1)
    y, z, c = spots()
    zp = [(y * NZ + lax.rem(z + d, NZ), c) for d in range(1, NZ)]
    yp = [(lax.rem(y + d, ny) * NZ + z, c) for d in range(1, ny)]
    cp = [(y * NZ + z, lax.rem(c + d, nc)) for d in range(1, nc)]
    plane = [(lax.rem(y + e, ny) * NZ + z, lax.rem(c + d, nc)) for e in range(ny) for d in range(nc) if e + d > 0]
    sync(zp + (plane if last else yp + cp))
    if last:
        ts = [remote(tot_ref, gott.at[z], st.at[d], rt.at[d], peer) for d, peer in enumerate(zp)]
    zs = [remote(cover_ref, gotz.at[z], sz.at[d], rz.at[d], peer) for d, peer in enumerate(zp)]
    cs = [remote(load_ref, gotc.at[c], sc.at[d], rc.at[d], peer) for d, peer in enumerate(cp)]
    gotz[z] = cover_ref[...]
    gotc[c] = load_ref[...]
    for cpy in cs:
        cpy.wait()
    total = gotc[0]
    for k in range(1, nc):
        total = total + gotc[k]
    mid[...] = total
    goty[y] = total
    ys = [remote(mid, goty.at[y], sy.at[d], ry.at[d], peer) for d, peer in enumerate(yp)]
    if last:
        gott[z] = tot_ref[...]
        for cpy in ts:
            cpy.wait()
        total = gott[0]
        for k in range(1, NZ):
            total = total + gott[k]
        midt[...] = total
        gotp[y * nc + c] = total
        ps = [remote(midt, gotp.at[y * nc + c], sp.at[d], rp.at[d], peer) for d, peer in enumerate(plane)]
    for cpy in zs:
        cpy.wait()
    cover = gotz[0]
    for k in range(1, NZ):
        cover = cover + gotz[k]
    lam = lam_ref[...] + size * wt_ref[...] * (1.0 - cover) / (1.0 + cover)
    if last:
        for r in range(NZ):
            own[r] = lam[r:r + 1]
            lam_out_ref[y * NZ + r] = lam[r:r + 1]
        ls = [remote(own, lam_out_ref.at[pl.ds(y * NZ, NZ)], sl.at[d], rl.at[d], peer) for d, peer in enumerate(yp)]
    else:
        lam_out_ref[...] = lam
    for cpy in ys:
        cpy.wait()
    load = goty[0]
    for k in range(1, ny):
        load = load + goty[k]
    for k in range(ny):
        row = slice(k, k + 1)
        valid = infos_ref[k, 0:1, :]
        cap = infos_ref[k, 3:4, :]
        got = load[row]
        mu = jnp.maximum(0.0, mu_ref[row, :] + size * (got - cap) / (got + jnp.where(valid > 0, cap, 1.0)))
        mu_out_ref[row, :] = mu * valid
    if last:
        for cpy in ps:
            cpy.wait()
        total = gotp[0]
        for k in range(1, ny * nc):
            total = total + gotp[k]
        tot_out_ref[...] = total
        for cpy in ls:
            cpy.wait()


def finish_kernel(total_cust, mu_ref, tot_ref, open_ref, shut_ref, out_ref, bound_ref):
    n = open_ref.shape[1]
    y, z, c = spots()
    rows = jnp.concatenate([v.astype(F32) for v in split3(mu_ref[pl.ds(y, 1), :])] + [jnp.zeros((13, n), F32)], axis=0).astype(BF16)
    got = jnp.dot(rows, onehot_of(open_ref[...]), preferred_element_type=F32)
    out_ref[...] = jnp.where(open_ref[...] > 0, got[0:1] + got[1:2] + got[2:3], shut_ref[...])
    bound_ref[...] = tot_ref[0:1, :] / total_cust


def params(cid=None, mib=24):
    return pltpu.CompilerParams(collective_id=cid, has_side_effects=True, vmem_limit_bytes=mib * 2 ** 20) if cid is not None else pltpu.CompilerParams(vmem_limit_bytes=mib * 2 ** 20)


def packed(kernel, *head):
    def run(*refs):
        kernel(*head, refs)
    return run


def local(nf, nc, fac_coords, cust_coords, open_flags, demand, fixed_cost, capacity, cap_mult, cover_mult):
    n, width = fac_coords.shape
    cols = cust_coords.shape[0]
    ny = nf // NZ
    total_cust = cols * nf * nc
    sd = jax.ShapeDtypeStruct
    dma = pltpu.SemaphoreType.DMA
    scr = pltpu.VMEM
    open_row = open_flags.reshape(1, n)
    comp, info, wt, lam, ext, shut = pl.pallas_call(
        pre_kernel,
        out_shape=(sd((n, width), BF16), sd((8, n), F32), sd((NZ, cols), F32), sd((NZ, cols), F32), sd((8, 128), F32), sd((1, n), F32)),
        in_specs=[VMEM] * 7, out_specs=(VMEM,) * 6, compiler_params=params(), name="pre",
    )(open_row, fac_coords, capacity.reshape(1, n), cap_mult.reshape(1, n), fixed_cost.reshape(1, n),
      demand.reshape(1, nf * cols), cover_mult.reshape(1, nf * cols))
    hops = NZ // 2
    cust, facs, infos = pl.pallas_call(
        functools.partial(gather_kernel, ny),
        out_shape=(sd((NZ, cols, width), BF16), sd((ny, n, width), BF16), sd((ny, 8, n), F32)),
        in_specs=[VMEM] * 3, out_specs=(VMEM,) * 3,
        scratch_shapes=[dma((2, hops, CHUNKS)), dma((2, hops, CHUNKS)), dma((ny - 1, 2)), dma((ny - 1, 2))],
        compiler_params=params(0), name="gather",
    )(cust_coords, comp, info)
    rows = ny * n + 3 * ROWS
    total = NZ * cols
    half = total // BLOCK // 2
    work = [
        scr((rows, 2 * width), BF16),
        scr((2 * width, total), BF16),
        scr((2, ROWS, BLOCK), F32),
        scr((2, ROWS, half * BLOCK), BF16),
        scr((total, 128), BF16),
        scr((rows + n, 128), F32),
        scr((8, total), F32),
        scr((8, total), F32),
    ]
    tot = ext
    mu = None
    for step in range(ITERS):
        last = step == ITERS - 1
        outs = (sd((ny, n), F32), sd((NZ, cols), F32), sd((8, 128), F32))
        if step == 0:
            load, cover, tot, mu, coords, turned, hq = pl.pallas_call(
                packed(step_kernel, step, ny),
                out_shape=outs + (sd((ny, n), F32), sd((rows, width), BF16), sd((width, total), BF16), sd((NZ, cols), F32)),
                in_specs=[VMEM] * 6, out_specs=(VMEM,) * 7, scratch_shapes=work, compiler_params=params(), name="step",
            )(facs, infos, cust, lam, wt, tot)
        else:
            load, cover, tot = pl.pallas_call(
                packed(step_kernel, step, ny),
                out_shape=outs, in_specs=[VMEM] * 8, out_specs=(VMEM,) * 3, scratch_shapes=work,
                compiler_params=params(), name="step",
            )(coords, infos, turned, hq, mu, lam, wt, tot)
        scratch = [scr((NZ, NZ, cols), F32), scr((nc, ny, n), F32), scr((ny, ny, n), F32), scr((ny, n), F32),
                   dma((NZ - 1,)), dma((NZ - 1,)), dma((nc - 1,)), dma((nc - 1,)), dma((ny - 1,)), dma((ny - 1,))]
        if not last:
            lam, mu = pl.pallas_call(
                packed(reduce_kernel, step, ny, nc),
                out_shape=(sd((NZ, cols), F32), sd((ny, n), F32)), in_specs=[VMEM] * 6, out_specs=(VMEM,) * 2,
                scratch_shapes=scratch, compiler_params=params(1 + step), name="reduce",
            )(load, cover, lam, wt, mu, infos)
        else:
            plane = ny * nc
            lam_all, mu, tot = pl.pallas_call(
                packed(reduce_kernel, step, ny, nc),
                out_shape=(sd((nf, 1, cols), F32), sd((ny, n), F32), sd((8, 128), F32)), in_specs=[VMEM] * 7, out_specs=(VMEM,) * 3,
                scratch_shapes=scratch + [scr((NZ, 8, 128), F32), scr((plane, 8, 128), F32), scr((8, 128), F32), scr((NZ, 1, cols), F32),
                                          dma((NZ - 1,)), dma((NZ - 1,)), dma((plane - 1,)), dma((plane - 1,)), dma((ny - 1,)), dma((ny - 1,))],
                compiler_params=params(1 + step), name="reduce",
            )(load, cover, lam, wt, mu, infos, tot)
    cap_final, bounds = pl.pallas_call(
        functools.partial(finish_kernel, total_cust), out_shape=(sd((1, n), F32), sd((1, 128), F32)),
        in_specs=[VMEM] * 4, out_specs=(VMEM,) * 2, compiler_params=params(), name="finish",
    )(mu, tot, open_row, shut)
    return lam_all.reshape(nf * cols), cap_final.reshape(n), bounds[0, :ITERS]


def solution(mesh):
    nf, nc = mesh.shape["fac"], mesh.shape["cust"]
    return jax.shard_map(
        functools.partial(local, nf, nc),
        mesh=mesh,
        in_specs=(P("fac", None), P(("cust", "fac"), None), P("fac"), P("cust"), P("fac"), P("fac"), P("fac"), P("cust")),
        out_specs=(P("cust"), P("fac"), P()),
        check_vma=False,
    )
```

```python
import functools
import math

import jax
import jax.numpy as jnp
from jax import lax
from jax.experimental import pallas as pl
from jax.experimental.pallas import tpu as pltpu
from jax.sharding import PartitionSpec as P

MESH = pl.DeviceIdType.MESH
ITERS = 3
TAU = 0.1
ALIGN = 16
ROWS = 160
BLOCK = 512
CHUNKS = 4
NZ = 8
F32 = jnp.float32
BF16 = jnp.bfloat16
VMEM = pl.BlockSpec(memory_space=pltpu.VMEM)


def split3(v):
    a = v.astype(BF16)
    r = v - a.astype(F32)
    b = r.astype(BF16)
    c = (r - b.astype(F32)).astype(BF16)
    return a, b, c


def onehot_of(open_row):
    n = open_row.shape[1]
    flags = jnp.broadcast_to(open_row.astype(F32), (16, n)).astype(BF16)
    tri = (lax.broadcasted_iota(jnp.int32, (n, n), 0) <= lax.broadcasted_iota(jnp.int32, (n, n), 1)).astype(F32).astype(BF16)
    pos = jnp.dot(flags, tri, preferred_element_type=F32)[0:1]
    pos = jnp.where(open_row > 0, pos - 1.0, -1.0).astype(jnp.int32)
    hit = lax.broadcasted_iota(jnp.int32, (n, n), 0) == pos
    return jnp.where(hit, 1.0, 0.0).astype(BF16)


def nt(a, b):
    return lax.dot_general(a, b, (((1,), (1,)), ((), ())), preferred_element_type=F32)


def tn(a, b):
    return lax.dot_general(a, b, (((0,), (0,)), ((), ())), preferred_element_type=F32)


def spots():
    f, c = lax.axis_index("fac"), lax.axis_index("cust")
    return f // NZ, lax.rem(f, NZ), c


def sync(peers):
    barrier = pltpu.get_barrier_semaphore()
    for peer in peers:
        pl.semaphore_signal(barrier, inc=1, device_id=peer, device_id_type=MESH)
    pl.semaphore_wait(barrier, len(peers))


def remote(src, dst, send, recv, peer):
    cpy = pltpu.make_async_remote_copy(src, dst, send, recv, device_id=peer, device_id_type=MESH)
    cpy.start()
    return cpy


def compact(opened, fac, mu, cap):
    n, width = fac.shape
    hot = onehot_of(opened)
    comp = jnp.dot(hot, fac, preferred_element_type=F32).astype(BF16)
    sq = fac.astype(F32) ** 2
    s1, s2, _ = split3(sq)
    ones = jnp.ones((16, width), BF16)
    half = -0.5 * (nt(ones, s1) + nt(ones, s2))[0:1]
    rows = [jnp.ones((1, n), BF16)]
    for v in (half, mu, cap):
        rows.extend(split3(v))
    rows = [r.astype(F32) for r in rows] + [jnp.zeros((6, n), F32)]
    got = nt(jnp.concatenate(rows, axis=0).astype(BF16), hot)
    rows = [got[0:1]] + [got[3 * m + 1:3 * m + 2] + got[3 * m + 2:3 * m + 3] + got[3 * m + 3:3 * m + 4] for m in range(3)]
    return comp, jnp.concatenate(rows + [jnp.zeros((4, n), F32)], axis=0)


def gather_kernel(ny, cust_ref, open_ref, fac_ref, cap_ref, mu_ref, fixed_ref, demand_ref, cover_ref,
                  all_ref, facs_ref, infos_ref, wt_ref, lam_ref, ext_ref, shut_ref, sz, rz, sy, ry):
    y, z, c = spots()
    nz, cols = wt_ref.shape
    hops = NZ // 2
    zp = [(y * NZ + lax.rem(z + s, NZ), c) for s in (1, NZ - 1)]
    yp = [(lax.rem(y + d, ny) * NZ + z, c) for d in range(1, ny)]
    part = cols // CHUNKS
    sync(zp + yp)

    def move(d, s, j):
        src = lax.rem(z + (NZ - s if d == 0 else s), NZ)
        at = pl.ds(j * part, part)
        a = cust_ref.at[at] if s == 0 else all_ref.at[src, at]
        return remote(a, all_ref.at[src, at], sz.at[d, s, j], rz.at[d, s, j], zp[d])

    def valid(d, s, j):
        return s < hops - 1 or (s == hops - 1 and (j < CHUNKS // 2) == (d == 0))

    ring = {}
    for j in range(CHUNKS):
        for d in range(2):
            if valid(d, 0, j):
                ring[d, 0, j] = move(d, 0, j)
    comp, info = compact(open_ref[...], fac_ref[...], mu_ref[...], cap_ref[...])
    facs_ref[y] = comp
    infos_ref[y] = info
    for r in range(nz):
        mine = pl.ds(pl.multiple_of((y * nz + r) * cols, cols), cols)
        wt_ref[r:r + 1, :] = demand_ref[:, mine].astype(F32)
        lam_ref[r:r + 1, :] = cover_ref[:, mine]
    opened = open_ref[...].astype(F32)
    shut = mu_ref[...]
    ext = jnp.zeros((1, 128), F32)
    lane = lax.broadcasted_iota(jnp.int32, (1, 128), 1)
    for k in range(ITERS):
        fixed = jnp.sum(opened * fixed_ref[...] - (1.0 - opened) * shut * cap_ref[...])
        ext = ext + jnp.where((lane == k) & (c == 0), fixed, 0.0)
        shut = jnp.maximum(0.0, shut - 0.1 / (k + 1))
    ext_ref[...] = ext
    shut_ref[...] = shut
    all_ref[z] = cust_ref[...]
    side = []
    for k, peer in enumerate(yp):
        side.append(remote(infos_ref.at[y], infos_ref.at[y], sy.at[k, 0], ry.at[k, 0], peer))
        side.append(remote(facs_ref.at[y], facs_ref.at[y], sy.at[k, 1], ry.at[k, 1], peer))
    for s in range(hops):
        for j in range(CHUNKS):
            for d in range(2):
                if valid(d, s, j):
                    ring[d, s, j].wait_recv()
                    if valid(d, s + 1, j):
                        ring[d, s + 1, j] = move(d, s + 1, j)
    for cpy in ring.values():
        cpy.wait_send()
    for cpy in side:
        cpy.wait()


def step_kernel(step, ny, refs):
    first = step == 0
    if first:
        (facs_ref, infos_ref, cust_ref, lam_ref, wt_ref, ext_ref,
         load_ref, cover_ref, tot_ref, mu_out_ref, coords_ref, turned_ref, hq_ref,
         a_ref, w_ref, y_ref, acc_ref, cov_ref, soft_ref, dw_ref, z_ref) = refs
    else:
        (coords_ref, infos_ref, turned_ref, hq_ref, mu_ref, lam_ref, wt_ref, ext_ref,
         load_ref, cover_ref, tot_ref,
         a_ref, w_ref, y_ref, acc_ref, cov_ref, soft_ref, dw_ref, z_ref) = refs
    n = infos_ref.shape[2]
    nz, cols = lam_ref.shape
    width = coords_ref.shape[1]
    total = nz * cols
    tiles = total // BLOCK
    me_y, me_z, c = spots()
    if first:
        eye = (lax.broadcasted_iota(jnp.int32, (width, width), 0) == lax.broadcasted_iota(jnp.int32, (width, width), 1)).astype(F32).astype(BF16)
        for r in range(nz):
            turned = nt(eye, cust_ref[r])
            w_ref[r, 0:width, :] = turned.astype(BF16)
            turned_ref[r] = turned.astype(BF16)
            hq_ref[r:r + 1, :] = 0.5 * jnp.sum(turned * turned, axis=0, keepdims=True)
    else:
        w_ref[:, 0:width, :] = turned_ref[...]
    wt = wt_ref[...]
    lam = lam_ref[...]
    a1, a2, a3 = split3(64.0 * lam - hq_ref[...])
    one_c = jnp.ones((3, cols), F32)
    for r in range(nz):
        row = slice(r, r + 1)
        at = slice(r * cols, (r + 1) * cols)
        mw = jnp.broadcast_to(-64.0 * wt[row], (3, cols))
        aug = jnp.concatenate([a1[row].astype(F32), a2[row].astype(F32), a3[row].astype(F32), one_c, mw, jnp.zeros((7, cols), F32)], axis=0)
        w_ref[r, width:width + 16, :] = aug.astype(BF16)
        dw_ref[:, at] = jnp.broadcast_to(wt[row], (8, cols))
    w_ref[:, width + 16:, :] = jnp.zeros((nz, width - 16, cols), BF16)
    cov_ref[...] = jnp.zeros_like(cov_ref)
    soft_ref[...] = jnp.zeros_like(soft_ref)
    lane = lax.broadcasted_iota(jnp.int32, (ROWS, width), 1)
    pad = jnp.where(lane == 3, -30000.0, 0.0).astype(BF16)
    sel = (lax.broadcasted_iota(jnp.int32, (16, width), 0) == lax.broadcasted_iota(jnp.int32, (16, width), 1)).astype(F32).astype(BF16)
    offs = []
    off = jnp.int32(0)
    one_r = jnp.ones((3, n), F32)
    if not first:
        a_ref[:, 0:width] = coords_ref[...]
    for s in range(ny):
        valid = infos_ref[s, 0:1, :]
        if first:
            mu = infos_ref[s, 2:3, :] * valid
            mu_out_ref[s:s + 1, :] = mu
        else:
            mu = mu_ref[s:s + 1, :]
        b = jnp.where(valid > 0, infos_ref[s, 1:2, :], -30000.0)
        parts = [p.astype(F32) for p in split3(b) + split3(mu)]
        rows = jnp.concatenate([one_r] + parts + [jnp.zeros((7, n), F32)], axis=0).astype(BF16)
        side = tn(rows, sel).astype(BF16)
        count = jnp.sum(valid).astype(jnp.int32)
        off = pl.multiple_of(off, ALIGN)
        offs.append(off)
        if first:
            a_ref[pl.ds(off, n), 0:width] = facs_ref[s]
        a_ref[pl.ds(off, n), width:2 * width] = side
        off = off + ((count + ALIGN - 1) // ALIGN) * ALIGN
    tail = pl.multiple_of(off, ALIGN)
    if first:
        a_ref[pl.ds(tail, ROWS), 0:width] = jnp.zeros((ROWS, width), BF16)
    a_ref[pl.ds(tail, ROWS), width:2 * width] = pad
    if first:
        coords_ref[...] = a_ref[:, 0:width]
    n_blocks = (off + ROWS - 1) // ROWS
    scale = math.log2(math.e) / 6.4

    def dot(base, t, out):
        out[t] = jnp.dot(a_ref[pl.ds(base, ROWS), :], w_ref[t], preferred_element_type=F32)

    def phase(i, cur, nxt):
        base = pl.multiple_of(i * ROWS, ROWS)
        for t in range(tiles):
            dot(pl.multiple_of(base + ROWS, ROWS), t, nxt)
            spans = [slice(t * BLOCK + q * 128, t * BLOCK + (q + 1) * 128) for q in range(BLOCK // 128)]
            covs = [cov_ref[:, at] for at in spans]
            softs = [soft_ref[:, at] for at in spans]
            for r in range(0, ROWS, 32):
                slots = [pl.ds(pl.multiple_of(base + (r + 8 * s), 8), 8) for s in range(4)]
                loads = [acc_ref[at, :] for at in slots] if t else [jnp.zeros((8, 128), F32)] * 4
                for q in range(BLOCK // 128):
                    dw = dw_ref[:, spans[q]]
                    es = [jnp.exp2(cur[t, r + 8 * s:r + 8 * s + 8, q * 128:(q + 1) * 128] * scale) for s in range(4)]
                    us = [1.0 + e for e in es]
                    p01 = us[0] * us[1]
                    p23 = us[2] * us[3]
                    r01 = dw / p01
                    r23 = dw / p23
                    xs = [es[0] * (us[1] * r01), es[1] * (us[0] * r01), es[2] * (us[3] * r23), es[3] * (us[2] * r23)]
                    loads = [a + x for a, x in zip(loads, xs)]
                    covs[q] = covs[q] + ((xs[0] + xs[1]) + (xs[2] + xs[3]))
                    softs[q] = softs[q] + jnp.log(p01 * p23)
                for s in range(4):
                    acc_ref[slots[s], :] = loads[s]
            for q in range(BLOCK // 128):
                cov_ref[:, spans[q]] = covs[q]
                soft_ref[:, spans[q]] = softs[q]

    def body(i, _):
        phase(2 * i, y_ref, z_ref)
        pl.when(2 * i + 1 < n_blocks)(lambda: phase(2 * i + 1, z_ref, y_ref))
        return 0

    for t in range(tiles):
        dot(0, t, y_ref)
    lax.fori_loop(0, (n_blocks + 1) // 2, body, 0)
    ones = jnp.ones((16, 128), BF16)
    for s in range(ny):
        for b in range(n // 128):
            at = pl.ds(pl.multiple_of(offs[s] + b * 128, ALIGN), 128)
            got = sum(nt(ones, p)[0:1] for p in split3(acc_ref[at, :]))
            load_ref[s:s + 1, b * 128:(b + 1) * 128] = jnp.where(infos_ref[s, 0:1, b * 128:(b + 1) * 128] > 0, got, 0.0)
    soft = 0.0
    for r in range(nz):
        at = slice(r * cols, (r + 1) * cols)
        cover_ref[r:r + 1, :] = jnp.sum(cov_ref[:, at], axis=0, keepdims=True) / wt[r:r + 1]
        soft = soft + soft_ref[:, at] * wt[r:r + 1]
    mu_all = mu_out_ref if first else mu_ref
    caps = infos_ref[me_y, 3:4, :]
    mine = jnp.sum(mu_all[pl.ds(me_y, 1), :] * caps)
    owned = jnp.sum(lam_ref[pl.ds(me_z, 1), :] * wt_ref[pl.ds(me_z, 1), :])
    here = owned - TAU * jnp.sum(soft) - jnp.where(c == 0, mine, 0.0)
    spot = lax.broadcasted_iota(jnp.int32, (1, 128), 1) == step
    tot_ref[...] = ext_ref[...] + jnp.where(spot, here, 0.0)


def far(n):
    return sorted(range(1, n), key=lambda d: -min(d, n - d))


def reduce_kernel(step, ny, nc, refs):
    last = step == ITERS - 1
    if last:
        (load_ref, cover_ref, lam_ref, wt_ref, mu_ref, infos_ref, tot_ref,
         lam_out_ref, mu_out_ref, tot_out_ref,
         gotz, gotc, goty, mid, sz, rz, sc, rc, sy, ry, gott, gotp, midt, own, st, rt, sp, rp, sl, rl) = refs
    else:
        (load_ref, cover_ref, lam_ref, wt_ref, mu_ref, infos_ref,
         lam_out_ref, mu_out_ref,
         gotz, gotc, goty, mid, sz, rz, sc, rc, sy, ry) = refs
    size = 0.1 / (step + 1)
    y, z, c = spots()
    zp = [(y * NZ + lax.rem(z + d, NZ), c) for d in far(NZ)]
    yp = [(lax.rem(y + d, ny) * NZ + z, c) for d in far(ny)]
    cp = [(y * NZ + z, lax.rem(c + d, nc)) for d in far(nc)]
    plane = [(lax.rem(y + e, ny) * NZ + z, lax.rem(c + d, nc)) for e in far(ny) + [0] for d in far(nc) + [0] if e + d > 0]
    sync(zp + (plane if last else yp + cp))
    if last:
        ts = [remote(tot_ref, gott.at[z], st.at[d], rt.at[d], peer) for d, peer in enumerate(zp)]
    zs = [remote(cover_ref, gotz.at[z], sz.at[d], rz.at[d], peer) for d, peer in enumerate(zp)]
    cs = [remote(load_ref, gotc.at[c], sc.at[d], rc.at[d], peer) for d, peer in enumerate(cp)]
    gotz[z] = cover_ref[...]
    gotc[c] = load_ref[...]
    for cpy in cs:
        cpy.wait()
    total = gotc[0]
    for k in range(1, nc):
        total = total + gotc[k]
    mid[...] = total
    goty[y] = total
    ys = [remote(mid, goty.at[y], sy.at[d], ry.at[d], peer) for d, peer in enumerate(yp)]
    if last:
        gott[z] = tot_ref[...]
        for cpy in ts:
            cpy.wait()
        total = gott[0]
        for k in range(1, NZ):
            total = total + gott[k]
        midt[...] = total
        gotp[y * nc + c] = total
        ps = [remote(midt, gotp.at[y * nc + c], sp.at[d], rp.at[d], peer) for d, peer in enumerate(plane)]
    for cpy in zs:
        cpy.wait()
    cover = gotz[0]
    for k in range(1, NZ):
        cover = cover + gotz[k]
    lam = lam_ref[...] + size * wt_ref[...] * (1.0 - cover) / (1.0 + cover)
    if last:
        for r in range(NZ):
            own[r] = lam[r:r + 1]
            lam_out_ref[y * NZ + r] = lam[r:r + 1]
        ls = [remote(own, lam_out_ref.at[pl.ds(y * NZ, NZ)], sl.at[d], rl.at[d], peer) for d, peer in enumerate(yp)]
    else:
        lam_out_ref[...] = lam
    for cpy in ys:
        cpy.wait()
    load = goty[0]
    for k in range(1, ny):
        load = load + goty[k]
    for k in range(ny):
        row = slice(k, k + 1)
        valid = infos_ref[k, 0:1, :]
        cap = infos_ref[k, 3:4, :]
        got = load[row]
        mu = jnp.maximum(0.0, mu_ref[row, :] + size * (got - cap) / (got + jnp.where(valid > 0, cap, 1.0)))
        mu_out_ref[row, :] = mu * valid
    if last:
        for cpy in ps:
            cpy.wait()
        total = gotp[0]
        for k in range(1, ny * nc):
            total = total + gotp[k]
        tot_out_ref[...] = total
        for cpy in ls:
            cpy.wait()


def finish_kernel(total_cust, mu_ref, tot_ref, open_ref, shut_ref, out_ref, bound_ref):
    n = open_ref.shape[1]
    y, z, c = spots()
    rows = jnp.concatenate([v.astype(F32) for v in split3(mu_ref[pl.ds(y, 1), :])] + [jnp.zeros((13, n), F32)], axis=0).astype(BF16)
    got = jnp.dot(rows, onehot_of(open_ref[...]), preferred_element_type=F32)
    out_ref[...] = jnp.where(open_ref[...] > 0, got[0:1] + got[1:2] + got[2:3], shut_ref[...])
    bound_ref[...] = tot_ref[...] / total_cust


def params(cid=None, mib=24):
    return pltpu.CompilerParams(collective_id=cid, has_side_effects=True, vmem_limit_bytes=mib * 2 ** 20) if cid is not None else pltpu.CompilerParams(vmem_limit_bytes=mib * 2 ** 20)


def packed(kernel, *head):
    def run(*refs):
        kernel(*head, refs)
    return run


def work_of(ny, n, cols, width):
    scr = pltpu.VMEM
    rows = ny * n + 3 * ROWS
    total = NZ * cols
    return rows, [
        scr((rows, 2 * width), BF16),
        scr((total // BLOCK, 2 * width, BLOCK), BF16),
        scr((total // BLOCK, ROWS, BLOCK), F32),
        scr((rows, 128), F32),
        scr((8, total), F32),
        scr((8, total), F32),
        scr((8, total), F32),
        scr((total // BLOCK, ROWS, BLOCK), F32),
    ]


def local(nf, nc, fac_coords, cust_coords, open_flags, demand, fixed_cost, capacity, cap_mult, cover_mult):
    n, width = fac_coords.shape
    cols = cust_coords.shape[0]
    ny = nf // NZ
    total_cust = cols * nf * nc
    sd = jax.ShapeDtypeStruct
    dma = pltpu.SemaphoreType.DMA
    scr = pltpu.VMEM
    open_row = open_flags.reshape(1, n)
    hops = NZ // 2
    cust, facs, infos, wt, lam, ext, shut = pl.pallas_call(
        functools.partial(gather_kernel, ny),
        out_shape=(sd((NZ, cols, width), BF16), sd((ny, n, width), BF16), sd((ny, 8, n), F32),
                   sd((NZ, cols), F32), sd((NZ, cols), F32), sd((1, 128), F32), sd((1, n), F32)),
        in_specs=[VMEM] * 8, out_specs=(VMEM,) * 7,
        scratch_shapes=[dma((2, hops, CHUNKS)), dma((2, hops, CHUNKS)), dma((ny - 1, 2)), dma((ny - 1, 2))],
        compiler_params=params(0), name="gather",
    )(cust_coords, open_row, fac_coords, capacity.reshape(1, n), cap_mult.reshape(1, n), fixed_cost.reshape(1, n),
      demand.reshape(1, nf * cols), cover_mult.reshape(1, nf * cols))
    rows, work = work_of(ny, n, cols, width)
    tot = ext
    mu = None
    for step in range(ITERS):
        last = step == ITERS - 1
        outs = (sd((ny, n), F32), sd((NZ, cols), F32), sd((1, 128), F32))
        if step == 0:
            load, cover, tot, mu, coords, turned, hq = pl.pallas_call(
                packed(step_kernel, step, ny),
                out_shape=outs + (sd((ny, n), F32), sd((rows, width), BF16), sd((NZ, width, cols), BF16), sd((NZ, cols), F32)),
                in_specs=[VMEM] * 6, out_specs=(VMEM,) * 7, scratch_shapes=work, compiler_params=params(), name="step",
            )(facs, infos, cust, lam, wt, tot)
        else:
            load, cover, tot = pl.pallas_call(
                packed(step_kernel, step, ny),
                out_shape=outs, in_specs=[VMEM] * 8, out_specs=(VMEM,) * 3, scratch_shapes=work,
                compiler_params=params(), name="step",
            )(coords, infos, turned, hq, mu, lam, wt, tot)
        scratch = [scr((NZ, NZ, cols), F32), scr((nc, ny, n), F32), scr((ny, ny, n), F32), scr((ny, n), F32),
                   dma((NZ - 1,)), dma((NZ - 1,)), dma((nc - 1,)), dma((nc - 1,)), dma((ny - 1,)), dma((ny - 1,))]
        if not last:
            lam, mu = pl.pallas_call(
                packed(reduce_kernel, step, ny, nc),
                out_shape=(sd((NZ, cols), F32), sd((ny, n), F32)), in_specs=[VMEM] * 6, out_specs=(VMEM,) * 2,
                scratch_shapes=scratch, compiler_params=params(1 + step), name="reduce",
            )(load, cover, lam, wt, mu, infos)
        else:
            plane = ny * nc
            lam_all, mu, tot = pl.pallas_call(
                packed(reduce_kernel, step, ny, nc),
                out_shape=(sd((nf, 1, cols), F32), sd((ny, n), F32), sd((1, 128), F32)), in_specs=[VMEM] * 7, out_specs=(VMEM,) * 3,
                scratch_shapes=scratch + [scr((NZ, 1, 128), F32), scr((plane, 1, 128), F32), scr((1, 128), F32), scr((NZ, 1, cols), F32),
                                          dma((NZ - 1,)), dma((NZ - 1,)), dma((plane - 1,)), dma((plane - 1,)), dma((ny - 1,)), dma((ny - 1,))],
                compiler_params=params(1 + step), name="reduce",
            )(load, cover, lam, wt, mu, infos, tot)
    cap_final, bounds = pl.pallas_call(
        functools.partial(finish_kernel, total_cust), out_shape=(sd((1, n), F32), sd((1, 128), F32)),
        in_specs=[VMEM] * 4, out_specs=(VMEM,) * 2, compiler_params=params(), name="finish",
    )(mu, tot, open_row, shut)
    return lam_all.reshape(nf * cols), cap_final.reshape(n), bounds[0, :ITERS]


def solution(mesh):
    nf, nc = mesh.shape["fac"], mesh.shape["cust"]
    return jax.shard_map(
        functools.partial(local, nf, nc),
        mesh=mesh,
        in_specs=(P("fac", None), P(("cust", "fac"), None), P("fac"), P("cust"), P("fac"), P("fac"), P("fac"), P("cust")),
        out_specs=(P("cust"), P("fac"), P()),
        check_vma=False,
    )
```

```python
import functools
import math

import jax
import jax.numpy as jnp
from jax import lax
from jax.experimental import pallas as pl
from jax.experimental.pallas import tpu as pltpu
from jax.sharding import PartitionSpec as P

MESH = pl.DeviceIdType.MESH
ITERS = 3
TAU = 0.1
ALIGN = 16
ROWS = 160
BLOCK = 512
CHUNKS = 8
NZ = 8
F32 = jnp.float32
BF16 = jnp.bfloat16
VMEM = pl.BlockSpec(memory_space=pltpu.VMEM)
HBM = pl.BlockSpec(memory_space=pltpu.HBM)


def split3(v):
    a = v.astype(BF16)
    r = v - a.astype(F32)
    b = r.astype(BF16)
    c = (r - b.astype(F32)).astype(BF16)
    return a, b, c


def onehot_of(open_row):
    n = open_row.shape[1]
    flags = jnp.broadcast_to(open_row.astype(F32), (16, n)).astype(BF16)
    tri = (lax.broadcasted_iota(jnp.int32, (n, n), 0) <= lax.broadcasted_iota(jnp.int32, (n, n), 1)).astype(F32).astype(BF16)
    pos = jnp.dot(flags, tri, preferred_element_type=F32)[0:1]
    pos = jnp.where(open_row > 0, pos - 1.0, -1.0).astype(jnp.int32)
    hit = lax.broadcasted_iota(jnp.int32, (n, n), 0) == pos
    return jnp.where(hit, 1.0, 0.0).astype(BF16)


def nt(a, b):
    return lax.dot_general(a, b, (((1,), (1,)), ((), ())), preferred_element_type=F32)


def tn(a, b):
    return lax.dot_general(a, b, (((0,), (0,)), ((), ())), preferred_element_type=F32)


def spots():
    f, c = lax.axis_index("fac"), lax.axis_index("cust")
    return f // NZ, lax.rem(f, NZ), c


def sync(peers):
    barrier = pltpu.get_barrier_semaphore()
    for peer in peers:
        pl.semaphore_signal(barrier, inc=1, device_id=peer, device_id_type=MESH)
    pl.semaphore_wait(barrier, len(peers))


def remote(src, dst, send, recv, peer):
    cpy = pltpu.make_async_remote_copy(src, dst, send, recv, device_id=peer, device_id_type=MESH)
    cpy.start()
    return cpy


def compact(opened, fac, mu, cap):
    n, width = fac.shape
    hot = onehot_of(opened)
    comp = jnp.dot(hot, fac, preferred_element_type=F32).astype(BF16)
    sq = fac.astype(F32) ** 2
    s1, s2, _ = split3(sq)
    ones = jnp.ones((16, width), BF16)
    half = -0.5 * (nt(ones, s1) + nt(ones, s2))[0:1]
    rows = [jnp.ones((1, n), BF16)]
    for v in (half, mu, cap):
        rows.extend(split3(v))
    rows = [r.astype(F32) for r in rows] + [jnp.zeros((6, n), F32)]
    got = nt(jnp.concatenate(rows, axis=0).astype(BF16), hot)
    rows = [got[0:1]] + [got[3 * m + 1:3 * m + 2] + got[3 * m + 2:3 * m + 3] + got[3 * m + 3:3 * m + 4] for m in range(3)]
    return comp, jnp.concatenate(rows + [jnp.zeros((4, n), F32)], axis=0)


def gather_kernel(ny, cust_hbm, open_hbm, fac_hbm, cap_hbm, mu_hbm, fixed_hbm, demand_hbm, cover_hbm,
                  all_ref, facs_ref, infos_ref, wt_ref, lam_ref, ext_ref, shut_ref,
                  open_ref, fac_ref, cap_ref, mu_ref, fixed_ref, demand_ref, cover_ref, sz, rz, sy, ry, loc):
    y, z, c = spots()
    nz, cols = wt_ref.shape
    hops = NZ // 2
    zp = [(y * NZ + lax.rem(z + s, NZ), c) for s in (1, NZ - 1)]
    yp = [(lax.rem(y + d, ny) * NZ + z, c) for d in range(1, ny)]
    part = cols // CHUNKS
    segment = pl.ds(pl.multiple_of(y * (nz * cols), nz * cols), nz * cols)
    pairs = [(cust_hbm, all_ref.at[z]), (fac_hbm, fac_ref), (open_hbm, open_ref), (cap_hbm, cap_ref), (mu_hbm, mu_ref),
             (fixed_hbm, fixed_ref), (demand_hbm.at[:, segment], demand_ref), (cover_hbm.at[:, segment], cover_ref)]
    own = [pltpu.make_async_copy(a, b, loc.at[k]) for k, (a, b) in enumerate(pairs)]
    for cpy in own:
        cpy.start()
    sync(zp + yp)

    def move(d, s, j):
        src = lax.rem(z + (NZ - s if d == 0 else s), NZ)
        at = pl.ds(j * part, part)
        return remote(all_ref.at[src, at], all_ref.at[src, at], sz.at[d, s, j], rz.at[d, s, j], zp[d])

    def valid(d, s, j):
        return s < hops - 1 or (s == hops - 1 and (j < CHUNKS // 2) == (d == 0))

    ring = {}
    own[0].wait()
    for j in range(CHUNKS):
        for d in range(2):
            if valid(d, 0, j):
                ring[d, 0, j] = move(d, 0, j)
    for cpy in own[1:]:
        cpy.wait()
    comp, info = compact(open_ref[...], fac_ref[...], mu_ref[...], cap_ref[...])
    facs_ref[y] = comp
    infos_ref[y] = info
    for r in range(nz):
        mine = slice(r * cols, (r + 1) * cols)
        wt_ref[r:r + 1, :] = demand_ref[:, mine].astype(F32)
        lam_ref[r:r + 1, :] = cover_ref[:, mine]
    opened = open_ref[...].astype(F32)
    shut = mu_ref[...]
    ext = jnp.zeros((1, 128), F32)
    lane = lax.broadcasted_iota(jnp.int32, (1, 128), 1)
    for k in range(ITERS):
        fixed = jnp.sum(opened * fixed_ref[...] - (1.0 - opened) * shut * cap_ref[...])
        ext = ext + jnp.where((lane == k) & (c == 0), fixed, 0.0)
        shut = jnp.maximum(0.0, shut - 0.1 / (k + 1))
    ext_ref[...] = ext
    shut_ref[...] = shut
    side = []
    for k, peer in enumerate(yp):
        side.append(remote(infos_ref.at[y], infos_ref.at[y], sy.at[k, 0], ry.at[k, 0], peer))
        side.append(remote(facs_ref.at[y], facs_ref.at[y], sy.at[k, 1], ry.at[k, 1], peer))
    for s in range(hops):
        for j in range(CHUNKS):
            for d in range(2):
                if valid(d, s, j):
                    ring[d, s, j].wait_recv()
                    if valid(d, s + 1, j):
                        ring[d, s + 1, j] = move(d, s + 1, j)
    for cpy in ring.values():
        cpy.wait_send()
    for cpy in side:
        cpy.wait()


def step_kernel(step, ny, refs):
    first = step == 0
    if first:
        (facs_ref, infos_ref, cust_ref, lam_ref, wt_ref, ext_ref,
         load_ref, cover_ref, tot_ref, mu_out_ref, coords_ref, turned_ref, hq_ref,
         a_ref, w_ref, y_ref, acc_ref, cov_ref, soft_ref, dw_ref, z_ref) = refs
    else:
        (coords_ref, infos_ref, turned_ref, hq_ref, mu_ref, lam_ref, wt_ref, ext_ref,
         load_ref, cover_ref, tot_ref,
         a_ref, w_ref, y_ref, acc_ref, cov_ref, soft_ref, dw_ref, z_ref) = refs
    n = infos_ref.shape[2]
    nz, cols = lam_ref.shape
    width = coords_ref.shape[1]
    total = nz * cols
    tiles = total // BLOCK
    me_y, me_z, c = spots()
    if first:
        eye = (lax.broadcasted_iota(jnp.int32, (width, width), 0) == lax.broadcasted_iota(jnp.int32, (width, width), 1)).astype(F32).astype(BF16)
        for r in range(nz):
            turned = nt(eye, cust_ref[r])
            w_ref[r, 0:width, :] = turned.astype(BF16)
            turned_ref[r] = turned.astype(BF16)
            hq_ref[r:r + 1, :] = 0.5 * jnp.sum(turned * turned, axis=0, keepdims=True)
    else:
        w_ref[:, 0:width, :] = turned_ref[...]
    wt = wt_ref[...]
    lam = lam_ref[...]
    a1, a2, a3 = split3(64.0 * lam - hq_ref[...])
    one_c = jnp.ones((3, cols), F32)
    for r in range(nz):
        row = slice(r, r + 1)
        at = slice(r * cols, (r + 1) * cols)
        mw = jnp.broadcast_to(-64.0 * wt[row], (3, cols))
        aug = jnp.concatenate([a1[row].astype(F32), a2[row].astype(F32), a3[row].astype(F32), one_c, mw, jnp.zeros((7, cols), F32)], axis=0)
        w_ref[r, width:width + 16, :] = aug.astype(BF16)
        dw_ref[:, at] = jnp.broadcast_to(wt[row], (8, cols))
    w_ref[:, width + 16:, :] = jnp.zeros((nz, width - 16, cols), BF16)
    cov_ref[...] = jnp.zeros_like(cov_ref)
    soft_ref[...] = jnp.zeros_like(soft_ref)
    lane = lax.broadcasted_iota(jnp.int32, (ROWS, width), 1)
    pad = jnp.where(lane == 3, -30000.0, 0.0).astype(BF16)
    sel = (lax.broadcasted_iota(jnp.int32, (16, width), 0) == lax.broadcasted_iota(jnp.int32, (16, width), 1)).astype(F32).astype(BF16)
    offs = []
    off = jnp.int32(0)
    one_r = jnp.ones((3, n), F32)
    if not first:
        a_ref[:, 0:width] = coords_ref[...]
    for s in range(ny):
        valid = infos_ref[s, 0:1, :]
        if first:
            mu = infos_ref[s, 2:3, :] * valid
            mu_out_ref[s:s + 1, :] = mu
        else:
            mu = mu_ref[s:s + 1, :]
        b = jnp.where(valid > 0, infos_ref[s, 1:2, :], -30000.0)
        parts = [p.astype(F32) for p in split3(b) + split3(mu)]
        rows = jnp.concatenate([one_r] + parts + [jnp.zeros((7, n), F32)], axis=0).astype(BF16)
        side = tn(rows, sel).astype(BF16)
        count = jnp.sum(valid).astype(jnp.int32)
        off = pl.multiple_of(off, ALIGN)
        offs.append(off)
        if first:
            a_ref[pl.ds(off, n), 0:width] = facs_ref[s]
        a_ref[pl.ds(off, n), width:2 * width] = side
        off = off + ((count + ALIGN - 1) // ALIGN) * ALIGN
    tail = pl.multiple_of(off, ALIGN)
    if first:
        a_ref[pl.ds(tail, ROWS), 0:width] = jnp.zeros((ROWS, width), BF16)
    a_ref[pl.ds(tail, ROWS), width:2 * width] = pad
    if first:
        coords_ref[...] = a_ref[:, 0:width]
    n_blocks = (off + ROWS - 1) // ROWS
    scale = math.log2(math.e) / 6.4

    def dot(base, t, out):
        out[t] = jnp.dot(a_ref[pl.ds(base, ROWS), :], w_ref[t], preferred_element_type=F32)

    def phase(i, cur, nxt, opening=False):
        base = pl.multiple_of(i * ROWS, ROWS)
        for t in range(tiles):
            if opening and t + 1 < tiles:
                dot(0, t + 1, cur)
            dot(pl.multiple_of(base + ROWS, ROWS), t, nxt)
            spans = [slice(t * BLOCK + q * 128, t * BLOCK + (q + 1) * 128) for q in range(BLOCK // 128)]
            covs = [cov_ref[:, at] for at in spans]
            softs = [soft_ref[:, at] for at in spans]
            for r in range(0, ROWS, 32):
                slots = [pl.ds(pl.multiple_of(base + (r + 8 * s), 8), 8) for s in range(4)]
                loads = [acc_ref[at, :] for at in slots] if t else [jnp.zeros((8, 128), F32)] * 4
                for q in range(BLOCK // 128):
                    dw = dw_ref[:, spans[q]]
                    es = [jnp.exp2(cur[t, r + 8 * s:r + 8 * s + 8, q * 128:(q + 1) * 128] * scale) for s in range(4)]
                    us = [1.0 + e for e in es]
                    p01 = us[0] * us[1]
                    p23 = us[2] * us[3]
                    r01 = dw / p01
                    r23 = dw / p23
                    xs = [es[0] * (us[1] * r01), es[1] * (us[0] * r01), es[2] * (us[3] * r23), es[3] * (us[2] * r23)]
                    loads = [a + x for a, x in zip(loads, xs)]
                    covs[q] = covs[q] + ((xs[0] + xs[1]) + (xs[2] + xs[3]))
                    softs[q] = softs[q] + jnp.log(p01 * p23)
                for s in range(4):
                    acc_ref[slots[s], :] = loads[s]
            for q in range(BLOCK // 128):
                cov_ref[:, spans[q]] = covs[q]
                soft_ref[:, spans[q]] = softs[q]

    def body(i, _):
        phase(2 * i + 1, z_ref, y_ref)
        pl.when(2 * i + 2 < n_blocks)(lambda: phase(2 * i + 2, y_ref, z_ref))
        return 0

    dot(0, 0, y_ref)
    phase(jnp.int32(0), y_ref, z_ref, True)
    lax.fori_loop(0, n_blocks // 2, body, 0)
    ones = jnp.ones((16, 128), BF16)
    for s in range(ny):
        for b in range(n // 128):
            at = pl.ds(pl.multiple_of(offs[s] + b * 128, ALIGN), 128)
            got = sum(nt(ones, p)[0:1] for p in split3(acc_ref[at, :])[:2])
            load_ref[s:s + 1, b * 128:(b + 1) * 128] = jnp.where(infos_ref[s, 0:1, b * 128:(b + 1) * 128] > 0, got, 0.0)
    soft = 0.0
    for r in range(nz):
        at = slice(r * cols, (r + 1) * cols)
        cover_ref[r:r + 1, :] = jnp.sum(cov_ref[:, at], axis=0, keepdims=True) / wt[r:r + 1]
        soft = soft + soft_ref[:, at] * wt[r:r + 1]
    mu_all = mu_out_ref if first else mu_ref
    caps = infos_ref[me_y, 3:4, :]
    mine = jnp.sum(mu_all[pl.ds(me_y, 1), :] * caps)
    owned = jnp.sum(lam_ref[pl.ds(me_z, 1), :] * wt_ref[pl.ds(me_z, 1), :])
    here = owned - TAU * jnp.sum(soft) - jnp.where(c == 0, mine, 0.0)
    spot = lax.broadcasted_iota(jnp.int32, (1, 128), 1) == step
    tot_ref[...] = ext_ref[...] + jnp.where(spot, here, 0.0)


def far(n):
    return sorted(range(1, n), key=lambda d: -min(d, n - d))


def reduce_kernel(step, ny, nc, refs):
    last = step == ITERS - 1
    if last:
        (load_ref, cover_ref, lam_ref, wt_ref, mu_ref, infos_ref, tot_ref, open_ref, shut_ref,
         lam_out_ref, cap_out_ref, bound_ref, mu_out_ref,
         gotz, gotc, goty, mid, sz, rz, sc, rc, sy, ry, gott, gotp, midt, own, st, rt, sp, rp, sl, rl) = refs
    else:
        (load_ref, cover_ref, lam_ref, wt_ref, mu_ref, infos_ref,
         lam_out_ref, mu_out_ref,
         gotz, gotc, goty, mid, sz, rz, sc, rc, sy, ry) = refs
    size = 0.1 / (step + 1)
    y, z, c = spots()
    zp = [(y * NZ + lax.rem(z + d, NZ), c) for d in far(NZ)]
    yp = [(lax.rem(y + d, ny) * NZ + z, c) for d in far(ny)]
    cp = [(y * NZ + z, lax.rem(c + d, nc)) for d in far(nc)]
    plane = [(lax.rem(y + e, ny) * NZ + z, lax.rem(c + d, nc)) for e in far(ny) + [0] for d in far(nc) + [0] if e + d > 0]
    sync(zp + (plane if last else yp + cp))
    if last:
        ts = [remote(tot_ref, gott.at[z], st.at[d], rt.at[d], peer) for d, peer in enumerate(zp)]
    zs = [remote(cover_ref, gotz.at[z], sz.at[d], rz.at[d], peer) for d, peer in enumerate(zp)]
    cs = [remote(load_ref, gotc.at[c], sc.at[d], rc.at[d], peer) for d, peer in enumerate(cp)]
    gotz[z] = cover_ref[...]
    gotc[c] = load_ref[...]
    for cpy in cs:
        cpy.wait()
    total = gotc[0]
    for k in range(1, nc):
        total = total + gotc[k]
    mid[...] = total
    goty[y] = total
    ys = [remote(mid, goty.at[y], sy.at[d], ry.at[d], peer) for d, peer in enumerate(yp)]
    if last:
        gott[z] = tot_ref[...]
        for cpy in ts:
            cpy.wait()
        total = gott[0]
        for k in range(1, NZ):
            total = total + gott[k]
        midt[...] = total
        gotp[y * nc + c] = total
        ps = [remote(midt, gotp.at[y * nc + c], sp.at[d], rp.at[d], peer) for d, peer in enumerate(plane)]
    for cpy in zs:
        cpy.wait()
    cover = gotz[0]
    for k in range(1, NZ):
        cover = cover + gotz[k]
    lam = lam_ref[...] + size * wt_ref[...] * (1.0 - cover) / (1.0 + cover)
    if last:
        for r in range(NZ):
            own[r] = lam[r:r + 1]
            lam_out_ref[y * NZ + r] = lam[r:r + 1]
        ls = [remote(own, lam_out_ref.at[pl.ds(y * NZ, NZ)], sl.at[d], rl.at[d], peer) for d, peer in enumerate(yp)]
    else:
        lam_out_ref[...] = lam
    for cpy in ys:
        cpy.wait()
    load = goty[0]
    for k in range(1, ny):
        load = load + goty[k]
    for k in range(ny):
        row = slice(k, k + 1)
        valid = infos_ref[k, 0:1, :]
        cap = infos_ref[k, 3:4, :]
        got = load[row]
        mu = jnp.maximum(0.0, mu_ref[row, :] + size * (got - cap) / (got + jnp.where(valid > 0, cap, 1.0)))
        mu_out_ref[row, :] = mu * valid
    if last:
        n = open_ref.shape[1]
        parts = [v.astype(F32) for v in split3(mu_out_ref[pl.ds(y, 1), :])]
        rows = jnp.concatenate(parts + [jnp.zeros((13, n), F32)], axis=0).astype(BF16)
        got = jnp.dot(rows, onehot_of(open_ref[...]), preferred_element_type=F32)
        cap_out_ref[...] = jnp.where(open_ref[...] > 0, got[0:1] + got[1:2] + got[2:3], shut_ref[...])
        for cpy in ps:
            cpy.wait()
        total = gotp[0]
        for k in range(1, ny * nc):
            total = total + gotp[k]
        bound_ref[...] = total / (NZ * ny * nc * lam_ref.shape[1])
        for cpy in ls:
            cpy.wait()


def params(cid=None, mib=24):
    return pltpu.CompilerParams(collective_id=cid, has_side_effects=True, vmem_limit_bytes=mib * 2 ** 20) if cid is not None else pltpu.CompilerParams(vmem_limit_bytes=mib * 2 ** 20)


def packed(kernel, *head):
    def run(*refs):
        kernel(*head, refs)
    return run


def work_of(ny, n, cols, width):
    scr = pltpu.VMEM
    rows = ny * n + 3 * ROWS
    total = NZ * cols
    return rows, [
        scr((rows, 2 * width), BF16),
        scr((total // BLOCK, 2 * width, BLOCK), BF16),
        scr((total // BLOCK, ROWS, BLOCK), F32),
        scr((rows, 128), F32),
        scr((8, total), F32),
        scr((8, total), F32),
        scr((8, total), F32),
        scr((total // BLOCK, ROWS, BLOCK), F32),
    ]


def local(nf, nc, fac_coords, cust_coords, open_flags, demand, fixed_cost, capacity, cap_mult, cover_mult):
    n, width = fac_coords.shape
    cols = cust_coords.shape[0]
    ny = nf // NZ
    sd = jax.ShapeDtypeStruct
    dma = pltpu.SemaphoreType.DMA
    scr = pltpu.VMEM
    open_row = open_flags.reshape(1, n)
    hops = NZ // 2
    cust, facs, infos, wt, lam, ext, shut = pl.pallas_call(
        functools.partial(gather_kernel, ny),
        out_shape=(sd((NZ, cols, width), BF16), sd((ny, n, width), BF16), sd((ny, 8, n), F32),
                   sd((NZ, cols), F32), sd((NZ, cols), F32), sd((1, 128), F32), sd((1, n), F32)),
        in_specs=[HBM] * 8, out_specs=(VMEM,) * 7,
        scratch_shapes=[scr((1, n), jnp.int32), scr((n, width), BF16), scr((1, n), F32), scr((1, n), F32), scr((1, n), F32),
                        scr((1, NZ * cols), jnp.int32), scr((1, NZ * cols), F32),
                        dma((2, hops, CHUNKS)), dma((2, hops, CHUNKS)), dma((ny - 1, 2)), dma((ny - 1, 2)), dma((8,))],
        compiler_params=params(0), name="gather",
    )(*[pltpu.with_memory_space_constraint(v, pltpu.HBM) for v in (
        cust_coords, open_row, fac_coords, capacity.reshape(1, n), cap_mult.reshape(1, n), fixed_cost.reshape(1, n),
        demand.reshape(1, nf * cols), cover_mult.reshape(1, nf * cols))])
    rows, work = work_of(ny, n, cols, width)
    tot = ext
    mu = None
    for step in range(ITERS):
        last = step == ITERS - 1
        outs = (sd((ny, n), F32), sd((NZ, cols), F32), sd((1, 128), F32))
        if step == 0:
            load, cover, tot, mu, coords, turned, hq = pl.pallas_call(
                packed(step_kernel, step, ny),
                out_shape=outs + (sd((ny, n), F32), sd((rows, width), BF16), sd((NZ, width, cols), BF16), sd((NZ, cols), F32)),
                in_specs=[VMEM] * 6, out_specs=(VMEM,) * 7, scratch_shapes=work, compiler_params=params(), name="step",
            )(facs, infos, cust, lam, wt, tot)
        else:
            load, cover, tot = pl.pallas_call(
                packed(step_kernel, step, ny),
                out_shape=outs, in_specs=[VMEM] * 8, out_specs=(VMEM,) * 3, scratch_shapes=work,
                compiler_params=params(), name="step",
            )(coords, infos, turned, hq, mu, lam, wt, tot)
        scratch = [scr((NZ, NZ, cols), F32), scr((nc, ny, n), F32), scr((ny, ny, n), F32), scr((ny, n), F32),
                   dma((NZ - 1,)), dma((NZ - 1,)), dma((nc - 1,)), dma((nc - 1,)), dma((ny - 1,)), dma((ny - 1,))]
        if not last:
            lam, mu = pl.pallas_call(
                packed(reduce_kernel, step, ny, nc),
                out_shape=(sd((NZ, cols), F32), sd((ny, n), F32)), in_specs=[VMEM] * 6, out_specs=(VMEM,) * 2,
                scratch_shapes=scratch, compiler_params=params(1 + step), name="reduce",
            )(load, cover, lam, wt, mu, infos)
        else:
            plane = ny * nc
            lam_all, cap_final, bounds = pl.pallas_call(
                packed(reduce_kernel, step, ny, nc),
                out_shape=(sd((nf, 1, cols), F32), sd((1, n), F32), sd((1, 128), F32)), in_specs=[VMEM] * 9, out_specs=(VMEM,) * 3,
                scratch_shapes=[scr((ny, n), F32)] + scratch + [
                    scr((NZ, 1, 128), F32), scr((plane, 1, 128), F32), scr((1, 128), F32), scr((NZ, 1, cols), F32),
                    dma((NZ - 1,)), dma((NZ - 1,)), dma((plane - 1,)), dma((plane - 1,)), dma((ny - 1,)), dma((ny - 1,))],
                compiler_params=params(1 + step), name="reduce",
            )(load, cover, lam, wt, mu, infos, tot, open_row, shut)
    return lam_all.reshape(nf * cols), cap_final.reshape(n), bounds[0, :ITERS]


def solution(mesh):
    nf, nc = mesh.shape["fac"], mesh.shape["cust"]
    return jax.shard_map(
        functools.partial(local, nf, nc),
        mesh=mesh,
        in_specs=(P("fac", None), P(("cust", "fac"), None), P("fac"), P("cust"), P("fac"), P("fac"), P("fac"), P("cust")),
        out_specs=(P("cust"), P("fac"), P()),
        check_vma=False,
    )
```

```python
import functools
import math

import jax
import jax.numpy as jnp
from jax import lax
from jax.experimental import pallas as pl
from jax.experimental.pallas import tpu as pltpu
from jax.sharding import PartitionSpec as P

MESH = pl.DeviceIdType.MESH
ITERS = 3
TAU = 0.1
ALIGN = 16
ROWS = 160
BLOCK = 512
CHUNKS = 8
NZ = 8
F32 = jnp.float32
BF16 = jnp.bfloat16
VMEM = pl.BlockSpec(memory_space=pltpu.VMEM)
HBM = pl.BlockSpec(memory_space=pltpu.HBM)


def split3(v):
    a = v.astype(BF16)
    r = v - a.astype(F32)
    b = r.astype(BF16)
    c = (r - b.astype(F32)).astype(BF16)
    return a, b, c


def onehot_of(open_row):
    n = open_row.shape[1]
    flags = jnp.broadcast_to(open_row.astype(F32), (16, n)).astype(BF16)
    tri = (lax.broadcasted_iota(jnp.int32, (n, n), 0) <= lax.broadcasted_iota(jnp.int32, (n, n), 1)).astype(F32).astype(BF16)
    pos = jnp.dot(flags, tri, preferred_element_type=F32)[0:1]
    pos = jnp.where(open_row > 0, pos - 1.0, -1.0).astype(jnp.int32)
    hit = lax.broadcasted_iota(jnp.int32, (n, n), 0) == pos
    return jnp.where(hit, 1.0, 0.0).astype(BF16)


def nt(a, b):
    return lax.dot_general(a, b, (((1,), (1,)), ((), ())), preferred_element_type=F32)


def tn(a, b):
    return lax.dot_general(a, b, (((0,), (0,)), ((), ())), preferred_element_type=F32)


def spots():
    f, c = lax.axis_index("fac"), lax.axis_index("cust")
    return f // NZ, lax.rem(f, NZ), c


def sync(peers):
    barrier = pltpu.get_barrier_semaphore()
    for peer in peers:
        pl.semaphore_signal(barrier, inc=1, device_id=peer, device_id_type=MESH)
    pl.semaphore_wait(barrier, len(peers))


def remote(src, dst, send, recv, peer):
    cpy = pltpu.make_async_remote_copy(src, dst, send, recv, device_id=peer, device_id_type=MESH)
    cpy.start()
    return cpy


def compact(opened, fac, mu, cap):
    n, width = fac.shape
    hot = onehot_of(opened)
    comp = jnp.dot(hot, fac, preferred_element_type=F32).astype(BF16)
    sq = fac.astype(F32) ** 2
    s1, s2, _ = split3(sq)
    ones = jnp.ones((16, width), BF16)
    half = -0.5 * (nt(ones, s1) + nt(ones, s2))[0:1]
    rows = [jnp.ones((1, n), BF16)]
    for v in (half, mu, cap):
        rows.extend(split3(v))
    rows = [r.astype(F32) for r in rows] + [jnp.zeros((6, n), F32)]
    got = nt(jnp.concatenate(rows, axis=0).astype(BF16), hot)
    rows = [got[0:1]] + [got[3 * m + 1:3 * m + 2] + got[3 * m + 2:3 * m + 3] + got[3 * m + 3:3 * m + 4] for m in range(3)]
    return comp, jnp.concatenate(rows + [jnp.zeros((4, n), F32)], axis=0)


def gather_kernel(ny, cust_hbm, open_hbm, fac_hbm, cap_hbm, mu_hbm, fixed_hbm, demand_hbm, cover_hbm,
                  facs_ref, infos_ref, wt_ref, lam_ref, ext_ref, shut_ref, flags_ref, turned_ref, hq_ref,
                  all_ref, open_ref, fac_ref, cap_ref, mu_ref, fixed_ref, demand_ref, cover_ref, sz, rz, sy, ry, loc):
    y, z, c = spots()
    nz, cols = wt_ref.shape
    hops = NZ // 2
    zp = [(y * NZ + lax.rem(z + s, NZ), c) for s in (1, NZ - 1)]
    yp = [(lax.rem(y + d, ny) * NZ + z, c) for d in range(1, ny)]
    part = cols // CHUNKS
    segment = pl.ds(pl.multiple_of(y * (nz * cols), nz * cols), nz * cols)
    pairs = [(cust_hbm, all_ref.at[z]), (fac_hbm, fac_ref), (open_hbm, open_ref), (cap_hbm, cap_ref), (mu_hbm, mu_ref),
             (fixed_hbm, fixed_ref), (demand_hbm.at[:, segment], demand_ref), (cover_hbm.at[:, segment], cover_ref)]
    own = [pltpu.make_async_copy(a, b, loc.at[k]) for k, (a, b) in enumerate(pairs)]
    for cpy in own:
        cpy.start()
    sync(zp + yp)

    def move(d, s, j):
        src = lax.rem(z + (NZ - s if d == 0 else s), NZ)
        at = pl.ds(j * part, part)
        return remote(all_ref.at[src, at], all_ref.at[src, at], sz.at[d, s, j], rz.at[d, s, j], zp[d])

    def valid(d, s, j):
        return s < hops - 1 or (s == hops - 1 and (j < CHUNKS // 2) == (d == 0))

    ring = {}
    own[0].wait()
    for j in range(CHUNKS):
        for d in range(2):
            if valid(d, 0, j):
                ring[d, 0, j] = move(d, 0, j)
    for cpy in own[1:]:
        cpy.wait()
    comp, info = compact(open_ref[...], fac_ref[...], mu_ref[...], cap_ref[...])
    facs_ref[y] = comp
    infos_ref[y] = info
    for r in range(nz):
        mine = slice(r * cols, (r + 1) * cols)
        wt_ref[r:r + 1, :] = demand_ref[:, mine].astype(F32)
        lam_ref[r:r + 1, :] = cover_ref[:, mine]
    opened = open_ref[...].astype(F32)
    shut = mu_ref[...]
    ext = jnp.zeros((1, 128), F32)
    lane = lax.broadcasted_iota(jnp.int32, (1, 128), 1)
    for k in range(ITERS):
        fixed = jnp.sum(opened * fixed_ref[...] - (1.0 - opened) * shut * cap_ref[...])
        ext = ext + jnp.where((lane == k) & (c == 0), fixed, 0.0)
        shut = jnp.maximum(0.0, shut - 0.1 / (k + 1))
    ext_ref[...] = ext
    shut_ref[...] = shut
    flags_ref[...] = open_ref[...]
    side = []
    for k, peer in enumerate(yp):
        side.append(remote(infos_ref.at[y], infos_ref.at[y], sy.at[k, 0], ry.at[k, 0], peer))
        side.append(remote(facs_ref.at[y], facs_ref.at[y], sy.at[k, 1], ry.at[k, 1], peer))
    width = fac_ref.shape[1]
    eye = (lax.broadcasted_iota(jnp.int32, (width, width), 0) == lax.broadcasted_iota(jnp.int32, (width, width), 1)).astype(F32).astype(BF16)

    def turn(k):
        turned = nt(eye, all_ref[k])
        turned_ref[k] = turned.astype(BF16)
        hq_ref[pl.ds(k, 1), :] = 0.5 * jnp.sum(turned * turned, axis=0, keepdims=True)

    turn(z)
    for s in range(hops):
        for j in range(CHUNKS):
            for d in range(2):
                if valid(d, s, j):
                    ring[d, s, j].wait_recv()
                    if valid(d, s + 1, j):
                        ring[d, s + 1, j] = move(d, s + 1, j)
        turn(lax.rem(z + s + 1, NZ))
        if s < hops - 1:
            turn(lax.rem(z + NZ - s - 1, NZ))
    for cpy in ring.values():
        cpy.wait_send()
    for cpy in side:
        cpy.wait()


def step_kernel(step, ny, refs):
    first = step == 0
    if first:
        (facs_ref, infos_ref, turned_ref, hq_ref, lam_ref, wt_ref, ext_ref,
         load_ref, cover_ref, tot_ref, mu_out_ref, coords_ref,
         a_ref, w_ref, y_ref, acc_ref, cov_ref, soft_ref, dw_ref, z_ref) = refs
    else:
        (coords_ref, infos_ref, turned_ref, hq_ref, mu_ref, lam_ref, wt_ref, ext_ref,
         load_ref, cover_ref, tot_ref,
         a_ref, w_ref, y_ref, acc_ref, cov_ref, soft_ref, dw_ref, z_ref) = refs
    n = infos_ref.shape[2]
    nz, cols = lam_ref.shape
    width = coords_ref.shape[1]
    total = nz * cols
    tiles = total // BLOCK
    me_y, me_z, c = spots()
    w_ref[:, 0:width, :] = turned_ref[...]
    wt = wt_ref[...]
    lam = lam_ref[...]
    a1, a2, a3 = split3(64.0 * lam - hq_ref[...])
    one_c = jnp.ones((3, cols), F32)
    for r in range(nz):
        row = slice(r, r + 1)
        at = slice(r * cols, (r + 1) * cols)
        mw = jnp.broadcast_to(-64.0 * wt[row], (3, cols))
        aug = jnp.concatenate([a1[row].astype(F32), a2[row].astype(F32), a3[row].astype(F32), one_c, mw, jnp.zeros((7, cols), F32)], axis=0)
        w_ref[r, width:width + 16, :] = aug.astype(BF16)
        dw_ref[:, at] = jnp.broadcast_to(wt[row], (8, cols))
    w_ref[:, width + 16:, :] = jnp.zeros((nz, width - 16, cols), BF16)
    cov_ref[...] = jnp.zeros_like(cov_ref)
    soft_ref[...] = jnp.zeros_like(soft_ref)
    lane = lax.broadcasted_iota(jnp.int32, (ROWS, width), 1)
    pad = jnp.where(lane == 3, -30000.0, 0.0).astype(BF16)
    sel = (lax.broadcasted_iota(jnp.int32, (16, width), 0) == lax.broadcasted_iota(jnp.int32, (16, width), 1)).astype(F32).astype(BF16)
    offs = []
    off = jnp.int32(0)
    one_r = jnp.ones((3, n), F32)
    if not first:
        a_ref[:, 0:width] = coords_ref[...]
    for s in range(ny):
        valid = infos_ref[s, 0:1, :]
        if first:
            mu = infos_ref[s, 2:3, :] * valid
            mu_out_ref[s:s + 1, :] = mu
        else:
            mu = mu_ref[s:s + 1, :]
        b = jnp.where(valid > 0, infos_ref[s, 1:2, :], -30000.0)
        parts = [p.astype(F32) for p in split3(b) + split3(mu)]
        rows = jnp.concatenate([one_r] + parts + [jnp.zeros((7, n), F32)], axis=0).astype(BF16)
        side = tn(rows, sel).astype(BF16)
        count = jnp.sum(valid).astype(jnp.int32)
        off = pl.multiple_of(off, ALIGN)
        offs.append(off)
        if first:
            a_ref[pl.ds(off, n), 0:width] = facs_ref[s]
        a_ref[pl.ds(off, n), width:2 * width] = side
        off = off + ((count + ALIGN - 1) // ALIGN) * ALIGN
    tail = pl.multiple_of(off, ALIGN)
    if first:
        a_ref[pl.ds(tail, ROWS), 0:width] = jnp.zeros((ROWS, width), BF16)
    a_ref[pl.ds(tail, ROWS), width:2 * width] = pad
    if first:
        coords_ref[...] = a_ref[:, 0:width]
    n_blocks = (off + ROWS - 1) // ROWS
    scale = math.log2(math.e) / 6.4

    def dot(base, t, out):
        out[t] = jnp.dot(a_ref[pl.ds(base, ROWS), :], w_ref[t], preferred_element_type=F32)

    def phase(i, cur, nxt, opening=False):
        base = pl.multiple_of(i * ROWS, ROWS)
        for t in range(tiles):
            if opening and t + 1 < tiles:
                dot(0, t + 1, cur)
            dot(pl.multiple_of(base + ROWS, ROWS), t, nxt)
            spans = [slice(t * BLOCK + q * 128, t * BLOCK + (q + 1) * 128) for q in range(BLOCK // 128)]
            covs = [cov_ref[:, at] for at in spans]
            softs = [soft_ref[:, at] for at in spans]
            for r in range(0, ROWS, 32):
                slots = [pl.ds(pl.multiple_of(base + (r + 8 * s), 8), 8) for s in range(4)]
                loads = [acc_ref[at, :] for at in slots] if t else [jnp.zeros((8, 128), F32)] * 4
                for q in range(BLOCK // 128):
                    dw = dw_ref[:, spans[q]]
                    es = [jnp.exp2(cur[t, r + 8 * s:r + 8 * s + 8, q * 128:(q + 1) * 128] * scale) for s in range(4)]
                    us = [1.0 + e for e in es]
                    p01 = us[0] * us[1]
                    p23 = us[2] * us[3]
                    r01 = dw / p01
                    r23 = dw / p23
                    xs = [es[0] * (us[1] * r01), es[1] * (us[0] * r01), es[2] * (us[3] * r23), es[3] * (us[2] * r23)]
                    loads = [a + x for a, x in zip(loads, xs)]
                    covs[q] = covs[q] + ((xs[0] + xs[1]) + (xs[2] + xs[3]))
                    softs[q] = softs[q] + jnp.log(p01 * p23)
                for s in range(4):
                    acc_ref[slots[s], :] = loads[s]
            for q in range(BLOCK // 128):
                cov_ref[:, spans[q]] = covs[q]
                soft_ref[:, spans[q]] = softs[q]

    def body(i, _):
        phase(2 * i + 1, z_ref, y_ref)
        pl.when(2 * i + 2 < n_blocks)(lambda: phase(2 * i + 2, y_ref, z_ref))
        return 0

    dot(0, 0, y_ref)
    phase(jnp.int32(0), y_ref, z_ref, True)
    lax.fori_loop(0, n_blocks // 2, body, 0)
    ones = jnp.ones((16, 128), BF16)
    for s in range(ny):
        for b in range(n // 128):
            at = pl.ds(pl.multiple_of(offs[s] + b * 128, ALIGN), 128)
            got = sum(nt(ones, p)[0:1] for p in split3(acc_ref[at, :])[:2])
            load_ref[s:s + 1, b * 128:(b + 1) * 128] = jnp.where(infos_ref[s, 0:1, b * 128:(b + 1) * 128] > 0, got, 0.0)
    soft = 0.0
    for r in range(nz):
        at = slice(r * cols, (r + 1) * cols)
        cover_ref[r:r + 1, :] = jnp.sum(cov_ref[:, at], axis=0, keepdims=True) / wt[r:r + 1]
        soft = soft + soft_ref[:, at] * wt[r:r + 1]
    mu_all = mu_out_ref if first else mu_ref
    caps = infos_ref[me_y, 3:4, :]
    mine = jnp.sum(mu_all[pl.ds(me_y, 1), :] * caps)
    owned = jnp.sum(lam_ref[pl.ds(me_z, 1), :] * wt_ref[pl.ds(me_z, 1), :])
    here = owned - TAU * jnp.sum(soft) - jnp.where(c == 0, mine, 0.0)
    spot = lax.broadcasted_iota(jnp.int32, (1, 128), 1) == step
    tot_ref[...] = ext_ref[...] + jnp.where(spot, here, 0.0)


def far(n):
    return sorted(range(1, n), key=lambda d: -min(d, n - d))


def reduce_kernel(step, ny, nc, refs):
    last = step == ITERS - 1
    if last:
        (load_ref, cover_ref, lam_ref, wt_ref, mu_ref, infos_ref, tot_ref, open_ref, shut_ref,
         lam_out_ref, cap_out_ref, bound_ref, mu_out_ref,
         gotz, gotc, goty, mid, sz, rz, sc, rc, sy, ry, gott, gotp, midt, own, st, rt, sp, rp, sl, rl) = refs
    else:
        (load_ref, cover_ref, lam_ref, wt_ref, mu_ref, infos_ref,
         lam_out_ref, mu_out_ref,
         gotz, gotc, goty, mid, sz, rz, sc, rc, sy, ry) = refs
    size = 0.1 / (step + 1)
    y, z, c = spots()
    zp = [(y * NZ + lax.rem(z + d, NZ), c) for d in far(NZ)]
    yp = [(lax.rem(y + d, ny) * NZ + z, c) for d in far(ny)]
    cp = [(y * NZ + z, lax.rem(c + d, nc)) for d in far(nc)]
    plane = [(lax.rem(y + e, ny) * NZ + z, lax.rem(c + d, nc)) for e in far(ny) + [0] for d in far(nc) + [0] if e + d > 0]
    sync(zp + (plane if last else yp + cp))
    if last:
        ts = [remote(tot_ref, gott.at[z], st.at[d], rt.at[d], peer) for d, peer in enumerate(zp)]
    zs = [remote(cover_ref, gotz.at[z], sz.at[d], rz.at[d], peer) for d, peer in enumerate(zp)]
    cs = [remote(load_ref, gotc.at[c], sc.at[d], rc.at[d], peer) for d, peer in enumerate(cp)]
    gotz[z] = cover_ref[...]
    gotc[c] = load_ref[...]
    for cpy in cs:
        cpy.wait_recv()
    total = gotc[0]
    for k in range(1, nc):
        total = total + gotc[k]
    mid[...] = total
    goty[y] = total
    ys = [remote(mid, goty.at[y], sy.at[d], ry.at[d], peer) for d, peer in enumerate(yp)]
    if last:
        gott[z] = tot_ref[...]
        for cpy in ts:
            cpy.wait_recv()
        total = gott[0]
        for k in range(1, NZ):
            total = total + gott[k]
        midt[...] = total
        gotp[y * nc + c] = total
        ps = [remote(midt, gotp.at[y * nc + c], sp.at[d], rp.at[d], peer) for d, peer in enumerate(plane)]
    for cpy in zs:
        cpy.wait_recv()
    cover = gotz[0]
    for k in range(1, NZ):
        cover = cover + gotz[k]
    lam = lam_ref[...] + size * wt_ref[...] * (1.0 - cover) / (1.0 + cover)
    if last:
        for r in range(NZ):
            own[r] = lam[r:r + 1]
            lam_out_ref[y * NZ + r] = lam[r:r + 1]
        ls = [remote(own, lam_out_ref.at[pl.ds(y * NZ, NZ)], sl.at[d], rl.at[d], peer) for d, peer in enumerate(yp)]
    else:
        lam_out_ref[...] = lam
    for cpy in ys:
        cpy.wait()
    load = goty[0]
    for k in range(1, ny):
        load = load + goty[k]
    for k in range(ny):
        row = slice(k, k + 1)
        valid = infos_ref[k, 0:1, :]
        cap = infos_ref[k, 3:4, :]
        got = load[row]
        mu = jnp.maximum(0.0, mu_ref[row, :] + size * (got - cap) / (got + jnp.where(valid > 0, cap, 1.0)))
        mu_out_ref[row, :] = mu * valid
    if last:
        n = open_ref.shape[1]
        parts = [v.astype(F32) for v in split3(mu_out_ref[pl.ds(y, 1), :])]
        rows = jnp.concatenate(parts + [jnp.zeros((13, n), F32)], axis=0).astype(BF16)
        got = jnp.dot(rows, onehot_of(open_ref[...]), preferred_element_type=F32)
        cap_out_ref[...] = jnp.where(open_ref[...] > 0, got[0:1] + got[1:2] + got[2:3], shut_ref[...])
        for cpy in ps:
            cpy.wait()
        total = gotp[0]
        for k in range(1, ny * nc):
            total = total + gotp[k]
        bound_ref[...] = total / (NZ * ny * nc * lam_ref.shape[1])
        for cpy in ls:
            cpy.wait()
        for cpy in ts:
            cpy.wait_send()
    for cpy in zs + cs:
        cpy.wait_send()


def finish_kernel(lam_ref, cap_ref, bound_ref, lam_out, cap_out, bound_out, sems):
    copies = [pltpu.make_async_copy(lam_ref, lam_out, sems.at[0]), pltpu.make_async_copy(cap_ref, cap_out, sems.at[1])]
    for cpy in copies:
        cpy.start()
    lane = lax.broadcasted_iota(jnp.int32, (1, 128), 1)
    for k in range(ITERS):
        bound_out[k] = jnp.sum(jnp.where(lane == k, bound_ref[...], 0.0))
    for cpy in copies:
        cpy.wait()


def params(cid=None, mib=24):
    return pltpu.CompilerParams(collective_id=cid, has_side_effects=True, vmem_limit_bytes=mib * 2 ** 20) if cid is not None else pltpu.CompilerParams(vmem_limit_bytes=mib * 2 ** 20)


def packed(kernel, *head):
    def run(*refs):
        kernel(*head, refs)
    return run


def work_of(ny, n, cols, width):
    scr = pltpu.VMEM
    rows = ny * n + 3 * ROWS
    total = NZ * cols
    return rows, [
        scr((rows, 2 * width), BF16),
        scr((total // BLOCK, 2 * width, BLOCK), BF16),
        scr((total // BLOCK, ROWS, BLOCK), F32),
        scr((rows, 128), F32),
        scr((8, total), F32),
        scr((8, total), F32),
        scr((8, total), F32),
        scr((total // BLOCK, ROWS, BLOCK), F32),
    ]


def local(nf, nc, fac_coords, cust_coords, open_flags, demand, fixed_cost, capacity, cap_mult, cover_mult):
    n, width = fac_coords.shape
    cols = cust_coords.shape[0]
    ny = nf // NZ
    sd = jax.ShapeDtypeStruct
    dma = pltpu.SemaphoreType.DMA
    scr = pltpu.VMEM
    open_row = open_flags.reshape(1, n)
    hops = NZ // 2
    facs, infos, wt, lam, ext, shut, flags, turned, hq = pl.pallas_call(
        functools.partial(gather_kernel, ny),
        out_shape=(sd((ny, n, width), BF16), sd((ny, 8, n), F32),
                   sd((NZ, cols), F32), sd((NZ, cols), F32), sd((1, 128), F32), sd((1, n), F32), sd((1, n), jnp.int32),
                   sd((NZ, width, cols), BF16), sd((NZ, cols), F32)),
        in_specs=[HBM] * 8, out_specs=(VMEM,) * 9,
        scratch_shapes=[scr((NZ, cols, width), BF16), scr((1, n), jnp.int32), scr((n, width), BF16), scr((1, n), F32), scr((1, n), F32), scr((1, n), F32),
                        scr((1, NZ * cols), jnp.int32), scr((1, NZ * cols), F32),
                        dma((2, hops, CHUNKS)), dma((2, hops, CHUNKS)), dma((ny - 1, 2)), dma((ny - 1, 2)), dma((8,))],
        compiler_params=params(0), name="gather",
    )(*[pltpu.with_memory_space_constraint(v, pltpu.HBM) for v in (
        cust_coords, open_row, fac_coords, capacity.reshape(1, n), cap_mult.reshape(1, n), fixed_cost.reshape(1, n),
        demand.reshape(1, nf * cols), cover_mult.reshape(1, nf * cols))])
    rows, work = work_of(ny, n, cols, width)
    tot = ext
    mu = None
    for step in range(ITERS):
        last = step == ITERS - 1
        outs = (sd((ny, n), F32), sd((NZ, cols), F32), sd((1, 128), F32))
        if step == 0:
            load, cover, tot, mu, coords = pl.pallas_call(
                packed(step_kernel, step, ny),
                out_shape=outs + (sd((ny, n), F32), sd((rows, width), BF16)),
                in_specs=[VMEM] * 7, out_specs=(VMEM,) * 5, scratch_shapes=work, compiler_params=params(), name="step",
            )(facs, infos, turned, hq, lam, wt, tot)
        else:
            load, cover, tot = pl.pallas_call(
                packed(step_kernel, step, ny),
                out_shape=outs, in_specs=[VMEM] * 8, out_specs=(VMEM,) * 3, scratch_shapes=work,
                compiler_params=params(), name="step",
            )(coords, infos, turned, hq, mu, lam, wt, tot)
        scratch = [scr((NZ, NZ, cols), F32), scr((nc, ny, n), F32), scr((ny, ny, n), F32), scr((ny, n), F32),
                   dma((NZ - 1,)), dma((NZ - 1,)), dma((nc - 1,)), dma((nc - 1,)), dma((ny - 1,)), dma((ny - 1,))]
        if not last:
            lam, mu = pl.pallas_call(
                packed(reduce_kernel, step, ny, nc),
                out_shape=(sd((NZ, cols), F32), sd((ny, n), F32)), in_specs=[VMEM] * 6, out_specs=(VMEM,) * 2,
                scratch_shapes=scratch, compiler_params=params(1 + step), name="reduce",
            )(load, cover, lam, wt, mu, infos)
        else:
            plane = ny * nc
            lam_all, cap_final, bounds = pl.pallas_call(
                packed(reduce_kernel, step, ny, nc),
                out_shape=(sd((nf, 1, cols), F32), sd((1, n), F32), sd((1, 128), F32)), in_specs=[VMEM] * 9, out_specs=(VMEM,) * 3,
                scratch_shapes=[scr((ny, n), F32)] + scratch + [
                    scr((NZ, 1, 128), F32), scr((plane, 1, 128), F32), scr((1, 128), F32), scr((NZ, 1, cols), F32),
                    dma((NZ - 1,)), dma((NZ - 1,)), dma((plane - 1,)), dma((plane - 1,)), dma((ny - 1,)), dma((ny - 1,))],
                compiler_params=params(1 + step), name="reduce",
            )(load, cover, lam, wt, mu, infos, tot, flags, shut)
    lam_all, cap_final, bounds = pl.pallas_call(
        finish_kernel, out_shape=(sd((nf, 1, cols), F32), sd((1, n), F32), sd((ITERS,), F32)),
        in_specs=[VMEM] * 3, out_specs=(HBM, HBM, pl.BlockSpec(memory_space=pltpu.SMEM)), scratch_shapes=[dma((2,))],
        compiler_params=params(), name="finish",
    )(lam_all, cap_final, bounds)
    return lam_all.reshape(nf * cols), cap_final.reshape(n), bounds


def solution(mesh):
    nf, nc = mesh.shape["fac"], mesh.shape["cust"]
    return jax.shard_map(
        functools.partial(local, nf, nc),
        mesh=mesh,
        in_specs=(P("fac", None), P(("cust", "fac"), None), P("fac"), P("cust"), P("fac"), P("fac"), P("fac"), P("cust")),
        out_specs=(P("cust"), P("fac"), P()),
        check_vma=False,
    )
```

```python
import functools
import math

import jax
import jax.numpy as jnp
from jax import lax
from jax.experimental import pallas as pl
from jax.experimental.pallas import tpu as pltpu
from jax.sharding import PartitionSpec as P

MESH = pl.DeviceIdType.MESH
ITERS = 3
TAU = 0.1
ALIGN = 16
ROWS = 160
HEAD = 160
BLOCK = 512
CHUNKS = 8
NZ = 8
F32 = jnp.float32
BF16 = jnp.bfloat16
VMEM = pl.BlockSpec(memory_space=pltpu.VMEM)
HBM = pl.BlockSpec(memory_space=pltpu.HBM)


def split3(v):
    a = v.astype(BF16)
    r = v - a.astype(F32)
    b = r.astype(BF16)
    c = (r - b.astype(F32)).astype(BF16)
    return a, b, c


def onehot_of(open_row):
    n = open_row.shape[1]
    flags = jnp.broadcast_to(open_row.astype(F32), (16, n)).astype(BF16)
    tri = (lax.broadcasted_iota(jnp.int32, (n, n), 0) <= lax.broadcasted_iota(jnp.int32, (n, n), 1)).astype(F32).astype(BF16)
    pos = jnp.dot(flags, tri, preferred_element_type=F32)[0:1]
    pos = jnp.where(open_row > 0, pos - 1.0, -1.0).astype(jnp.int32)
    hit = lax.broadcasted_iota(jnp.int32, (n, n), 0) == pos
    return jnp.where(hit, 1.0, 0.0).astype(BF16)


def nt(a, b):
    return lax.dot_general(a, b, (((1,), (1,)), ((), ())), preferred_element_type=F32)


def tn(a, b):
    return lax.dot_general(a, b, (((0,), (0,)), ((), ())), preferred_element_type=F32)


def spots():
    f, c = lax.axis_index("fac"), lax.axis_index("cust")
    return f // NZ, lax.rem(f, NZ), c


def greet(peers):
    barrier = pltpu.get_barrier_semaphore()
    for peer in peers:
        pl.semaphore_signal(barrier, inc=1, device_id=peer, device_id_type=MESH)


def sync(peers):
    greet(peers)
    pl.semaphore_wait(pltpu.get_barrier_semaphore(), len(peers))


def remote(src, dst, send, recv, peer):
    cpy = pltpu.make_async_remote_copy(src, dst, send, recv, device_id=peer, device_id_type=MESH)
    cpy.start()
    return cpy


def compact(opened, fac, mu, cap):
    n, width = fac.shape
    hot = onehot_of(opened)
    comp = jnp.dot(hot, fac, preferred_element_type=F32).astype(BF16)
    sq = fac.astype(F32) ** 2
    s1, s2, _ = split3(sq)
    ones = jnp.ones((16, width), BF16)
    half = -0.5 * (nt(ones, s1) + nt(ones, s2))[0:1]
    rows = [jnp.ones((1, n), BF16)]
    for v in (half, mu, cap):
        rows.extend(split3(v))
    rows = [r.astype(F32) for r in rows] + [jnp.zeros((6, n), F32)]
    got = nt(jnp.concatenate(rows, axis=0).astype(BF16), hot)
    rows = [got[0:1]] + [got[3 * m + 1:3 * m + 2] + got[3 * m + 2:3 * m + 3] + got[3 * m + 3:3 * m + 4] for m in range(3)]
    return comp, jnp.concatenate(rows + [jnp.zeros((4, n), F32)], axis=0)


def gather_kernel(ny, cust_hbm, open_hbm, fac_hbm, cap_hbm, mu_hbm, fixed_hbm, demand_hbm, cover_hbm,
                  facs_ref, infos_ref, wt_ref, lam_ref, ext_ref, shut_ref, flags_ref, turned_ref, hq_ref,
                  all_ref, open_ref, fac_ref, cap_ref, mu_ref, fixed_ref, demand_ref, cover_ref, sz, rz, sy, ry, loc):
    y, z, c = spots()
    nz, cols = wt_ref.shape
    hops = NZ // 2
    zp = [(y * NZ + lax.rem(z + s, NZ), c) for s in (1, NZ - 1)]
    yp = [(lax.rem(y + d, ny) * NZ + z, c) for d in range(1, ny)]
    part = cols // CHUNKS
    segment = pl.ds(pl.multiple_of(y * (nz * cols), nz * cols), nz * cols)
    pairs = [(cust_hbm, all_ref.at[z]), (fac_hbm, fac_ref), (open_hbm, open_ref), (cap_hbm, cap_ref), (mu_hbm, mu_ref),
             (fixed_hbm, fixed_ref), (demand_hbm.at[:, segment], demand_ref), (cover_hbm.at[:, segment], cover_ref)]
    own = [pltpu.make_async_copy(a, b, loc.at[k]) for k, (a, b) in enumerate(pairs)]
    for cpy in own:
        cpy.start()
    sync(zp + yp)

    def move(d, s, j):
        src = lax.rem(z + (NZ - s if d == 0 else s), NZ)
        at = pl.ds(j * part, part)
        return remote(all_ref.at[src, at], all_ref.at[src, at], sz.at[d, s, j], rz.at[d, s, j], zp[d])

    def valid(d, s, j):
        return s < hops - 1 or (s == hops - 1 and (j < CHUNKS // 2) == (d == 0))

    ring = {}
    own[0].wait()
    for j in range(CHUNKS):
        for d in range(2):
            if valid(d, 0, j):
                ring[d, 0, j] = move(d, 0, j)
    for cpy in own[1:]:
        cpy.wait()
    comp, info = compact(open_ref[...], fac_ref[...], mu_ref[...], cap_ref[...])
    facs_ref[y] = comp
    infos_ref[y] = info
    for r in range(nz):
        mine = slice(r * cols, (r + 1) * cols)
        wt_ref[r:r + 1, :] = demand_ref[:, mine].astype(F32)
        lam_ref[r:r + 1, :] = cover_ref[:, mine]
    opened = open_ref[...].astype(F32)
    shut = mu_ref[...]
    ext = jnp.zeros((1, 128), F32)
    lane = lax.broadcasted_iota(jnp.int32, (1, 128), 1)
    for k in range(ITERS):
        fixed = jnp.sum(opened * fixed_ref[...] - (1.0 - opened) * shut * cap_ref[...])
        ext = ext + jnp.where((lane == k) & (c == 0), fixed, 0.0)
        shut = jnp.maximum(0.0, shut - 0.1 / (k + 1))
    ext_ref[...] = ext
    shut_ref[...] = shut
    flags_ref[...] = open_ref[...]
    side = []
    for k, peer in enumerate(yp):
        side.append(remote(infos_ref.at[y], infos_ref.at[y], sy.at[k, 0], ry.at[k, 0], peer))
        side.append(remote(facs_ref.at[y], facs_ref.at[y], sy.at[k, 1], ry.at[k, 1], peer))
    width = fac_ref.shape[1]
    eye = (lax.broadcasted_iota(jnp.int32, (width, width), 0) == lax.broadcasted_iota(jnp.int32, (width, width), 1)).astype(F32).astype(BF16)

    def turn(k):
        turned = nt(eye, all_ref[k])
        turned_ref[k] = turned.astype(BF16)
        hq_ref[pl.ds(k, 1), :] = 0.5 * jnp.sum(turned * turned, axis=0, keepdims=True)

    turn(z)
    for s in range(hops):
        for j in range(CHUNKS):
            for d in range(2):
                if valid(d, s, j):
                    ring[d, s, j].wait_recv()
                    if valid(d, s + 1, j):
                        ring[d, s + 1, j] = move(d, s + 1, j)
        turn(lax.rem(z + s + 1, NZ))
        if s < hops - 1:
            turn(lax.rem(z + NZ - s - 1, NZ))
    for cpy in ring.values():
        cpy.wait_send()
    for cpy in side:
        cpy.wait()


def step_kernel(step, ny, refs):
    first = step == 0
    if first:
        (facs_ref, infos_ref, turned_ref, hq_ref, lam_ref, wt_ref, ext_ref,
         load_ref, cover_ref, tot_ref, w_ref, head_ref, mu_out_ref, coords_ref,
         a_ref, y_ref, acc_ref, cov_ref, soft_ref, dw_ref, z_ref) = refs
    else:
        (coords_ref, infos_ref, turned_ref, hq_ref, mu_ref, lam_ref, wt_ref, ext_ref,
         load_ref, cover_ref, tot_ref, w_ref, head_ref,
         a_ref, y_ref, acc_ref, cov_ref, soft_ref, dw_ref, z_ref) = refs
    n = infos_ref.shape[2]
    nz, cols = lam_ref.shape
    width = coords_ref.shape[1]
    total = nz * cols
    tiles = total // BLOCK
    me_y, me_z, c = spots()
    w_ref[:, 0:width, :] = turned_ref[...]
    wt = wt_ref[...]
    lam = lam_ref[...]
    a1, a2, a3 = split3(64.0 * lam - hq_ref[...])
    one_c = jnp.ones((3, cols), F32)
    for r in range(nz):
        row = slice(r, r + 1)
        at = slice(r * cols, (r + 1) * cols)
        mw = jnp.broadcast_to(-64.0 * wt[row], (3, cols))
        aug = jnp.concatenate([a1[row].astype(F32), a2[row].astype(F32), a3[row].astype(F32), one_c, mw, jnp.zeros((7, cols), F32)], axis=0)
        w_ref[r, width:width + 16, :] = aug.astype(BF16)
        dw_ref[:, at] = jnp.broadcast_to(wt[row], (8, cols))
    w_ref[:, width + 16:, :] = jnp.zeros((nz, width - 16, cols), BF16)
    cov_ref[...] = jnp.zeros_like(cov_ref)
    soft_ref[...] = jnp.zeros_like(soft_ref)
    lane = lax.broadcasted_iota(jnp.int32, (ROWS, width), 1)
    pad = jnp.where(lane == 3, -30000.0, 0.0).astype(BF16)
    sel = (lax.broadcasted_iota(jnp.int32, (16, width), 0) == lax.broadcasted_iota(jnp.int32, (16, width), 1)).astype(F32).astype(BF16)
    offs = []
    off = jnp.int32(0)
    one_r = jnp.ones((3, n), F32)
    if not first:
        a_ref[:, 0:width] = coords_ref[...]
    for s in range(ny):
        valid = infos_ref[s, 0:1, :]
        if first:
            mu = infos_ref[s, 2:3, :] * valid
            mu_out_ref[s:s + 1, :] = mu
        else:
            mu = mu_ref[s:s + 1, :]
        b = jnp.where(valid > 0, infos_ref[s, 1:2, :], -30000.0)
        parts = [p.astype(F32) for p in split3(b) + split3(mu)]
        rows = jnp.concatenate([one_r] + parts + [jnp.zeros((7, n), F32)], axis=0).astype(BF16)
        side = tn(rows, sel).astype(BF16)
        count = jnp.sum(valid).astype(jnp.int32)
        off = pl.multiple_of(off, ALIGN)
        offs.append(off)
        if first:
            a_ref[pl.ds(off, n), 0:width] = facs_ref[s]
        a_ref[pl.ds(off, n), width:2 * width] = side
        off = off + ((count + ALIGN - 1) // ALIGN) * ALIGN
        if s == 0:
            off = jnp.maximum(off, HEAD)
    tail = pl.multiple_of(off, ALIGN)
    if first:
        a_ref[pl.ds(tail, ROWS), 0:width] = jnp.zeros((ROWS, width), BF16)
    a_ref[pl.ds(tail, ROWS), width:2 * width] = pad
    if first:
        coords_ref[...] = a_ref[:, 0:width]
    head_ref[...] = a_ref[0:HEAD, :]
    n_blocks = (off - HEAD + ROWS - 1) // ROWS
    scale = math.log2(math.e) / 6.4

    def dot(base, t, out):
        out[t] = jnp.dot(a_ref[pl.ds(base, ROWS), :], w_ref[t], preferred_element_type=F32)

    def phase(i, cur, nxt, opening=False):
        base = pl.multiple_of(HEAD + i * ROWS, 32)
        for t in range(tiles):
            if opening and t + 1 < tiles:
                dot(HEAD, t + 1, cur)
            dot(pl.multiple_of(base + ROWS, 32), t, nxt)
            spans = [slice(t * BLOCK + q * 128, t * BLOCK + (q + 1) * 128) for q in range(BLOCK // 128)]
            covs = [cov_ref[:, at] for at in spans]
            softs = [soft_ref[:, at] for at in spans]
            for r in range(0, ROWS, 32):
                slots = [pl.ds(pl.multiple_of(base + (r + 8 * s), 8), 8) for s in range(4)]
                loads = [acc_ref[at, :] for at in slots] if t else [jnp.zeros((8, 128), F32)] * 4
                for q in range(BLOCK // 128):
                    dw = dw_ref[:, spans[q]]
                    es = [jnp.exp2(cur[t, r + 8 * s:r + 8 * s + 8, q * 128:(q + 1) * 128] * scale) for s in range(4)]
                    us = [1.0 + e for e in es]
                    p01 = us[0] * us[1]
                    p23 = us[2] * us[3]
                    r01 = dw / p01
                    r23 = dw / p23
                    xs = [es[0] * (us[1] * r01), es[1] * (us[0] * r01), es[2] * (us[3] * r23), es[3] * (us[2] * r23)]
                    loads = [a + x for a, x in zip(loads, xs)]
                    covs[q] = covs[q] + ((xs[0] + xs[1]) + (xs[2] + xs[3]))
                    softs[q] = softs[q] + jnp.log(p01 * p23)
                for s in range(4):
                    acc_ref[slots[s], :] = loads[s]
            for q in range(BLOCK // 128):
                cov_ref[:, spans[q]] = covs[q]
                soft_ref[:, spans[q]] = softs[q]

    def body(i, _):
        phase(2 * i + 1, z_ref, y_ref)
        pl.when(2 * i + 2 < n_blocks)(lambda: phase(2 * i + 2, y_ref, z_ref))
        return 0

    dot(HEAD, 0, y_ref)
    acc_ref[0:HEAD, :] = jnp.zeros((HEAD, 128), F32)
    phase(jnp.int32(0), y_ref, z_ref, True)
    lax.fori_loop(0, n_blocks // 2, body, 0)
    ones = jnp.ones((16, 128), BF16)
    for s in range(ny):
        for b in range(n // 128):
            at = pl.ds(pl.multiple_of(offs[s] + b * 128, ALIGN), 128)
            got = sum(nt(ones, p)[0:1] for p in split3(acc_ref[at, :])[:2])
            load_ref[s:s + 1, b * 128:(b + 1) * 128] = jnp.where(infos_ref[s, 0:1, b * 128:(b + 1) * 128] > 0, got, 0.0)
    soft = 0.0
    for r in range(nz):
        at = slice(r * cols, (r + 1) * cols)
        cover_ref[r:r + 1, :] = jnp.sum(cov_ref[:, at], axis=0, keepdims=True)
        soft = soft + soft_ref[:, at] * wt[r:r + 1]
    mu_all = mu_out_ref if first else mu_ref
    caps = infos_ref[me_y, 3:4, :]
    mine = jnp.sum(mu_all[pl.ds(me_y, 1), :] * caps)
    owned = jnp.sum(lam_ref[pl.ds(me_z, 1), :] * wt_ref[pl.ds(me_z, 1), :])
    here = owned - TAU * jnp.sum(soft) - jnp.where(c == 0, mine, 0.0)
    spot = lax.broadcasted_iota(jnp.int32, (1, 128), 1) == step
    tot_ref[...] = ext_ref[...] + jnp.where(spot, here, 0.0)


def head_rows(wt_ref, w_ref, head_ref, hy, hacc, hcov):
    tiles = w_ref.shape[0]
    scale = math.log2(math.e) / 6.4
    for t in range(tiles):
        hy[t] = jnp.dot(head_ref[...], w_ref[t], preferred_element_type=F32)
    hacc[...] = jnp.zeros_like(hacc)

    def body(t, soft):
        covs = [jnp.zeros((16, 128), F32)] * (BLOCK // 128)
        softs = [jnp.zeros((8, 128), F32)] * (BLOCK // 128)
        weights = wt_ref[pl.ds(t, 1), :]
        for r in range(0, HEAD, 32):
            loads = [hacc[r:r + 16, :], hacc[r + 16:r + 32, :]]
            for q in range(BLOCK // 128):
                at = slice(q * 128, (q + 1) * 128)
                es = [jnp.exp2(hy[t, r + 16 * s:r + 16 * s + 16, at] * scale) for s in range(2)]
                us = [1.0 + e for e in es]
                p = us[0] * us[1]
                inv = weights[:, at] / p
                xs = [es[0] * (us[1] * inv), es[1] * (us[0] * inv)]
                loads = [a + x for a, x in zip(loads, xs)]
                covs[q] = covs[q] + (xs[0] + xs[1])
                softs[q] = softs[q] + jnp.log(p[0:8] * p[8:16])
            hacc[r:r + 16, :] = loads[0]
            hacc[r + 16:r + 32, :] = loads[1]
        hcov[pl.ds(t, 1), :] = jnp.concatenate([jnp.sum(v, axis=0, keepdims=True) for v in covs], axis=1)
        for q in range(BLOCK // 128):
            soft = soft + softs[q] * weights[:, q * 128:(q + 1) * 128]
        return soft

    return jnp.sum(lax.fori_loop(0, tiles, body, jnp.zeros((8, 128), F32)))


def far(n):
    return sorted(range(1, n), key=lambda d: -min(d, n - d))


def reduce_kernel(step, ny, nc, refs):
    last = step == ITERS - 1
    if last:
        (load_ref, cover_ref, lam_ref, wt_ref, mu_ref, infos_ref, tot_ref, w_ref, head_ref, open_ref, shut_ref,
         lam_out_ref, cap_out_ref, bound_ref, mu_out_ref, tot_out_ref, hy, hacc, hcov, hload,
         gotz, gotc, goty, mid, sz, rz, sc, rc, sy, ry, gott, gotp, midt, own, st, rt, sp, rp, sl, rl) = refs
    else:
        (load_ref, cover_ref, lam_ref, wt_ref, mu_ref, infos_ref, tot_ref, w_ref, head_ref,
         lam_out_ref, mu_out_ref, tot_out_ref, hy, hacc, hcov, hload,
         gotz, gotc, goty, mid, sz, rz, sc, rc, sy, ry) = refs
    size = 0.1 / (step + 1)
    y, z, c = spots()
    zp = [(y * NZ + lax.rem(z + d, NZ), c) for d in far(NZ)]
    yp = [(lax.rem(y + d, ny) * NZ + z, c) for d in far(ny)]
    cp = [(y * NZ + z, lax.rem(c + d, nc)) for d in far(nc)]
    plane = [(lax.rem(y + e, ny) * NZ + z, lax.rem(c + d, nc)) for e in far(ny) + [0] for d in far(nc) + [0] if e + d > 0]
    peers = zp + (plane if last else yp + cp)
    greet(peers)
    tot_out_ref[...] = tot_ref[...] - jnp.where(lax.broadcasted_iota(jnp.int32, (1, 128), 1) == step, TAU * head_rows(wt_ref, w_ref, head_ref, hy, hacc, hcov), 0.0)
    gotz[z] = (cover_ref[...] + hcov[...]) / wt_ref[...]
    ones = jnp.ones((16, 128), BF16)
    hload[...] = load_ref[...]
    for b in range(2):
        at = slice(b * 128, (b + 1) * 128)
        hload[0:1, at] = load_ref[0:1, at] + sum(nt(ones, p)[0:1] for p in split3(hacc[at, :])[:2])
    gotc[c] = hload[...]
    pl.semaphore_wait(pltpu.get_barrier_semaphore(), len(peers))
    if last:
        ts = [remote(tot_out_ref, gott.at[z], st.at[d], rt.at[d], peer) for d, peer in enumerate(zp)]
    zs = [remote(gotz.at[z], gotz.at[z], sz.at[d], rz.at[d], peer) for d, peer in enumerate(zp)]
    cs = [remote(gotc.at[c], gotc.at[c], sc.at[d], rc.at[d], peer) for d, peer in enumerate(cp)]
    for cpy in cs:
        cpy.wait_recv()
    total = gotc[0]
    for k in range(1, nc):
        total = total + gotc[k]
    mid[...] = total
    goty[y] = total
    ys = [remote(mid, goty.at[y], sy.at[d], ry.at[d], peer) for d, peer in enumerate(yp)]
    if last:
        gott[z] = tot_out_ref[...]
        for cpy in ts:
            cpy.wait_recv()
        total = gott[0]
        for k in range(1, NZ):
            total = total + gott[k]
        midt[...] = total
        gotp[y * nc + c] = total
        ps = [remote(midt, gotp.at[y * nc + c], sp.at[d], rp.at[d], peer) for d, peer in enumerate(plane)]
    for cpy in zs:
        cpy.wait_recv()
    cover = gotz[0]
    for k in range(1, NZ):
        cover = cover + gotz[k]
    lam = lam_ref[...] + size * wt_ref[...] * (1.0 - cover) / (1.0 + cover)
    if last:
        for r in range(NZ):
            own[r] = lam[r:r + 1]
            lam_out_ref[y * NZ + r] = lam[r:r + 1]
        ls = [remote(own, lam_out_ref.at[pl.ds(y * NZ, NZ)], sl.at[d], rl.at[d], peer) for d, peer in enumerate(yp)]
    else:
        lam_out_ref[...] = lam
    for cpy in ys:
        cpy.wait()
    load = goty[0]
    for k in range(1, ny):
        load = load + goty[k]
    for k in range(ny):
        row = slice(k, k + 1)
        valid = infos_ref[k, 0:1, :]
        cap = infos_ref[k, 3:4, :]
        got = load[row]
        mu = jnp.maximum(0.0, mu_ref[row, :] + size * (got - cap) / (got + jnp.where(valid > 0, cap, 1.0)))
        mu_out_ref[row, :] = mu * valid
    if last:
        n = open_ref.shape[1]
        parts = [v.astype(F32) for v in split3(mu_out_ref[pl.ds(y, 1), :])]
        rows = jnp.concatenate(parts + [jnp.zeros((13, n), F32)], axis=0).astype(BF16)
        got = jnp.dot(rows, onehot_of(open_ref[...]), preferred_element_type=F32)
        cap_out_ref[...] = jnp.where(open_ref[...] > 0, got[0:1] + got[1:2] + got[2:3], shut_ref[...])
        for cpy in ps:
            cpy.wait()
        total = gotp[0]
        for k in range(1, ny * nc):
            total = total + gotp[k]
        bound_ref[...] = total / (NZ * ny * nc * lam_ref.shape[1])
        for cpy in ls:
            cpy.wait()
        for cpy in ts:
            cpy.wait_send()
    for cpy in zs + cs:
        cpy.wait_send()


def finish_kernel(lam_ref, cap_ref, bound_ref, lam_out, cap_out, bound_out, sems):
    copies = [pltpu.make_async_copy(lam_ref, lam_out, sems.at[0]), pltpu.make_async_copy(cap_ref, cap_out, sems.at[1])]
    for cpy in copies:
        cpy.start()
    lane = lax.broadcasted_iota(jnp.int32, (1, 128), 1)
    for k in range(ITERS):
        bound_out[k] = jnp.sum(jnp.where(lane == k, bound_ref[...], 0.0))
    for cpy in copies:
        cpy.wait()


def params(cid=None, mib=24):
    return pltpu.CompilerParams(collective_id=cid, has_side_effects=True, vmem_limit_bytes=mib * 2 ** 20) if cid is not None else pltpu.CompilerParams(vmem_limit_bytes=mib * 2 ** 20)


def packed(kernel, *head):
    def run(*refs):
        kernel(*head, refs)
    return run


def work_of(ny, n, cols, width):
    scr = pltpu.VMEM
    rows = ny * n + HEAD + 3 * ROWS
    total = NZ * cols
    return rows, [
        scr((rows, 2 * width), BF16),
        scr((total // BLOCK, ROWS, BLOCK), F32),
        scr((rows, 128), F32),
        scr((8, total), F32),
        scr((8, total), F32),
        scr((8, total), F32),
        scr((total // BLOCK, ROWS, BLOCK), F32),
    ]


def local(nf, nc, fac_coords, cust_coords, open_flags, demand, fixed_cost, capacity, cap_mult, cover_mult):
    n, width = fac_coords.shape
    cols = cust_coords.shape[0]
    ny = nf // NZ
    sd = jax.ShapeDtypeStruct
    dma = pltpu.SemaphoreType.DMA
    scr = pltpu.VMEM
    open_row = open_flags.reshape(1, n)
    hops = NZ // 2
    facs, infos, wt, lam, ext, shut, flags, turned, hq = pl.pallas_call(
        functools.partial(gather_kernel, ny),
        out_shape=(sd((ny, n, width), BF16), sd((ny, 8, n), F32),
                   sd((NZ, cols), F32), sd((NZ, cols), F32), sd((1, 128), F32), sd((1, n), F32), sd((1, n), jnp.int32),
                   sd((NZ, width, cols), BF16), sd((NZ, cols), F32)),
        in_specs=[HBM] * 8, out_specs=(VMEM,) * 9,
        scratch_shapes=[scr((NZ, cols, width), BF16), scr((1, n), jnp.int32), scr((n, width), BF16), scr((1, n), F32), scr((1, n), F32), scr((1, n), F32),
                        scr((1, NZ * cols), jnp.int32), scr((1, NZ * cols), F32),
                        dma((2, hops, CHUNKS)), dma((2, hops, CHUNKS)), dma((ny - 1, 2)), dma((ny - 1, 2)), dma((8,))],
        compiler_params=params(0), name="gather",
    )(*[pltpu.with_memory_space_constraint(v, pltpu.HBM) for v in (
        cust_coords, open_row, fac_coords, capacity.reshape(1, n), cap_mult.reshape(1, n), fixed_cost.reshape(1, n),
        demand.reshape(1, nf * cols), cover_mult.reshape(1, nf * cols))])
    rows, work = work_of(ny, n, cols, width)
    tot = ext
    mu = None
    for step in range(ITERS):
        last = step == ITERS - 1
        outs = (sd((ny, n), F32), sd((NZ, cols), F32), sd((1, 128), F32), sd((NZ, 2 * width, cols), BF16), sd((HEAD, 2 * width), BF16))
        if step == 0:
            load, cover, tot, w, head, mu, coords = pl.pallas_call(
                packed(step_kernel, step, ny),
                out_shape=outs + (sd((ny, n), F32), sd((rows, width), BF16)),
                in_specs=[VMEM] * 7, out_specs=(VMEM,) * 7, scratch_shapes=work, compiler_params=params(), name="step",
            )(facs, infos, turned, hq, lam, wt, tot)
        else:
            load, cover, tot, w, head = pl.pallas_call(
                packed(step_kernel, step, ny),
                out_shape=outs, in_specs=[VMEM] * 8, out_specs=(VMEM,) * 5, scratch_shapes=work,
                compiler_params=params(), name="step",
            )(coords, infos, turned, hq, mu, lam, wt, tot)
        front = [scr((NZ, HEAD, cols), F32), scr((256, 128), F32), scr((NZ, cols), F32), scr((ny, n), F32)]
        scratch = [scr((NZ, NZ, cols), F32), scr((nc, ny, n), F32), scr((ny, ny, n), F32), scr((ny, n), F32),
                   dma((NZ - 1,)), dma((NZ - 1,)), dma((nc - 1,)), dma((nc - 1,)), dma((ny - 1,)), dma((ny - 1,))]
        if not last:
            lam, mu, tot = pl.pallas_call(
                packed(reduce_kernel, step, ny, nc),
                out_shape=(sd((NZ, cols), F32), sd((ny, n), F32), sd((1, 128), F32)), in_specs=[VMEM] * 9, out_specs=(VMEM,) * 3,
                scratch_shapes=front + scratch, compiler_params=params(1 + step), name="reduce",
            )(load, cover, lam, wt, mu, infos, tot, w, head)
        else:
            plane = ny * nc
            lam_all, cap_final, bounds = pl.pallas_call(
                packed(reduce_kernel, step, ny, nc),
                out_shape=(sd((nf, 1, cols), F32), sd((1, n), F32), sd((1, 128), F32)), in_specs=[VMEM] * 11, out_specs=(VMEM,) * 3,
                scratch_shapes=[scr((ny, n), F32), scr((1, 128), F32)] + front + scratch + [
                    scr((NZ, 1, 128), F32), scr((plane, 1, 128), F32), scr((1, 128), F32), scr((NZ, 1, cols), F32),
                    dma((NZ - 1,)), dma((NZ - 1,)), dma((plane - 1,)), dma((plane - 1,)), dma((ny - 1,)), dma((ny - 1,))],
                compiler_params=params(1 + step), name="reduce",
            )(load, cover, lam, wt, mu, infos, tot, w, head, flags, shut)
    lam_all, cap_final, bounds = pl.pallas_call(
        finish_kernel, out_shape=(sd((nf, 1, cols), F32), sd((1, n), F32), sd((ITERS,), F32)),
        in_specs=[VMEM] * 3, out_specs=(HBM, HBM, pl.BlockSpec(memory_space=pltpu.SMEM)), scratch_shapes=[dma((2,))],
        compiler_params=params(), name="finish",
    )(lam_all, cap_final, bounds)
    return lam_all.reshape(nf * cols), cap_final.reshape(n), bounds


def solution(mesh):
    nf, nc = mesh.shape["fac"], mesh.shape["cust"]
    return jax.shard_map(
        functools.partial(local, nf, nc),
        mesh=mesh,
        in_specs=(P("fac", None), P(("cust", "fac"), None), P("fac"), P("cust"), P("fac"), P("fac"), P("fac"), P("cust")),
        out_specs=(P("cust"), P("fac"), P()),
        check_vma=False,
    )
```

```python
import functools
import math

import jax
import jax.numpy as jnp
from jax import lax
from jax.experimental import pallas as pl
from jax.experimental.pallas import tpu as pltpu
from jax.sharding import PartitionSpec as P

MESH = pl.DeviceIdType.MESH
ITERS = 3
TAU = 0.1
ALIGN = 16
ROWS = 160
HEAD = 80
BLOCK = 512
CHUNKS = 8
NZ = 8
F32 = jnp.float32
BF16 = jnp.bfloat16
VMEM = pl.BlockSpec(memory_space=pltpu.VMEM)
HBM = pl.BlockSpec(memory_space=pltpu.HBM)


def split3(v):
    a = v.astype(BF16)
    r = v - a.astype(F32)
    b = r.astype(BF16)
    c = (r - b.astype(F32)).astype(BF16)
    return a, b, c


def onehot_of(open_row):
    n = open_row.shape[1]
    flags = jnp.broadcast_to(open_row.astype(F32), (16, n)).astype(BF16)
    tri = (lax.broadcasted_iota(jnp.int32, (n, n), 0) <= lax.broadcasted_iota(jnp.int32, (n, n), 1)).astype(F32).astype(BF16)
    pos = jnp.dot(flags, tri, preferred_element_type=F32)[0:1]
    pos = jnp.where(open_row > 0, pos - 1.0, -1.0).astype(jnp.int32)
    hit = lax.broadcasted_iota(jnp.int32, (n, n), 0) == pos
    return jnp.where(hit, 1.0, 0.0).astype(BF16)


def nt(a, b):
    return lax.dot_general(a, b, (((1,), (1,)), ((), ())), preferred_element_type=F32)


def tn(a, b):
    return lax.dot_general(a, b, (((0,), (0,)), ((), ())), preferred_element_type=F32)


def spots():
    f, c = lax.axis_index("fac"), lax.axis_index("cust")
    return f // NZ, lax.rem(f, NZ), c


def greet(peers):
    barrier = pltpu.get_barrier_semaphore()
    for peer in peers:
        pl.semaphore_signal(barrier, inc=1, device_id=peer, device_id_type=MESH)


def sync(peers):
    greet(peers)
    pl.semaphore_wait(pltpu.get_barrier_semaphore(), len(peers))


def remote(src, dst, send, recv, peer):
    cpy = pltpu.make_async_remote_copy(src, dst, send, recv, device_id=peer, device_id_type=MESH)
    cpy.start()
    return cpy


def compact(opened, fac, mu, cap):
    n, width = fac.shape
    hot = onehot_of(opened)
    comp = jnp.dot(hot, fac, preferred_element_type=F32).astype(BF16)
    sq = fac.astype(F32) ** 2
    s1, s2, _ = split3(sq)
    ones = jnp.ones((16, width), BF16)
    half = -0.5 * (nt(ones, s1) + nt(ones, s2))[0:1]
    rows = [jnp.ones((1, n), BF16)]
    for v in (half, mu, cap):
        rows.extend(split3(v))
    rows = [r.astype(F32) for r in rows] + [jnp.zeros((6, n), F32)]
    got = nt(jnp.concatenate(rows, axis=0).astype(BF16), hot)
    rows = [got[0:1]] + [got[3 * m + 1:3 * m + 2] + got[3 * m + 2:3 * m + 3] + got[3 * m + 3:3 * m + 4] for m in range(3)]
    return comp, jnp.concatenate(rows + [jnp.zeros((4, n), F32)], axis=0)


def gather_kernel(ny, cust_hbm, open_hbm, fac_hbm, cap_hbm, mu_hbm, fixed_hbm, demand_hbm, cover_hbm,
                  facs_ref, infos_ref, wt_ref, lam_ref, ext_ref, shut_ref, flags_ref, turned_ref, hq_ref,
                  all_ref, open_ref, fac_ref, cap_ref, mu_ref, fixed_ref, demand_ref, cover_ref, sz, rz, sy, ry, loc):
    y, z, c = spots()
    nz, cols = wt_ref.shape
    hops = NZ // 2
    zp = [(y * NZ + lax.rem(z + s, NZ), c) for s in (1, NZ - 1)]
    yp = [(lax.rem(y + d, ny) * NZ + z, c) for d in range(1, ny)]
    part = cols // CHUNKS
    segment = pl.ds(pl.multiple_of(y * (nz * cols), nz * cols), nz * cols)
    pairs = [(cust_hbm, all_ref.at[z]), (fac_hbm, fac_ref), (open_hbm, open_ref), (cap_hbm, cap_ref), (mu_hbm, mu_ref),
             (fixed_hbm, fixed_ref), (demand_hbm.at[:, segment], demand_ref), (cover_hbm.at[:, segment], cover_ref)]
    own = [pltpu.make_async_copy(a, b, loc.at[k]) for k, (a, b) in enumerate(pairs)]
    for cpy in own:
        cpy.start()
    sync(zp + yp)

    def move(d, s, j):
        src = lax.rem(z + (NZ - s if d == 0 else s), NZ)
        at = pl.ds(j * part, part)
        return remote(all_ref.at[src, at], all_ref.at[src, at], sz.at[d, s, j], rz.at[d, s, j], zp[d])

    def valid(d, s, j):
        return s < hops - 1 or (s == hops - 1 and (j < CHUNKS // 2) == (d == 0))

    ring = {}
    own[0].wait()
    for j in range(CHUNKS):
        for d in range(2):
            if valid(d, 0, j):
                ring[d, 0, j] = move(d, 0, j)
    for cpy in own[1:]:
        cpy.wait()
    comp, info = compact(open_ref[...], fac_ref[...], mu_ref[...], cap_ref[...])
    facs_ref[y] = comp
    infos_ref[y] = info
    for r in range(nz):
        mine = slice(r * cols, (r + 1) * cols)
        wt_ref[r:r + 1, :] = demand_ref[:, mine].astype(F32)
        lam_ref[r:r + 1, :] = cover_ref[:, mine]
    opened = open_ref[...].astype(F32)
    shut = mu_ref[...]
    ext = jnp.zeros((1, 128), F32)
    lane = lax.broadcasted_iota(jnp.int32, (1, 128), 1)
    for k in range(ITERS):
        fixed = jnp.sum(opened * fixed_ref[...] - (1.0 - opened) * shut * cap_ref[...])
        ext = ext + jnp.where((lane == k) & (c == 0), fixed, 0.0)
        shut = jnp.maximum(0.0, shut - 0.1 / (k + 1))
    ext_ref[...] = ext
    shut_ref[...] = shut
    flags_ref[...] = open_ref[...]
    side = []
    for k, peer in enumerate(yp):
        side.append(remote(infos_ref.at[y], infos_ref.at[y], sy.at[k, 0], ry.at[k, 0], peer))
        side.append(remote(facs_ref.at[y], facs_ref.at[y], sy.at[k, 1], ry.at[k, 1], peer))
    width = fac_ref.shape[1]
    eye = (lax.broadcasted_iota(jnp.int32, (width, width), 0) == lax.broadcasted_iota(jnp.int32, (width, width), 1)).astype(F32).astype(BF16)

    def turn(k):
        turned = nt(eye, all_ref[k])
        turned_ref[k] = turned.astype(BF16)
        hq_ref[pl.ds(k, 1), :] = 0.5 * jnp.sum(turned * turned, axis=0, keepdims=True)

    turn(z)
    for s in range(hops):
        for j in range(CHUNKS):
            for d in range(2):
                if valid(d, s, j):
                    ring[d, s, j].wait_recv()
                    if valid(d, s + 1, j):
                        ring[d, s + 1, j] = move(d, s + 1, j)
        turn(lax.rem(z + s + 1, NZ))
        if s < hops - 1:
            turn(lax.rem(z + NZ - s - 1, NZ))
    for cpy in ring.values():
        cpy.wait_send()
    for cpy in side:
        cpy.wait()


def step_kernel(step, ny, refs):
    first = step == 0
    if first:
        (facs_ref, infos_ref, turned_ref, hq_ref, lam_ref, wt_ref, ext_ref,
         load_ref, cover_ref, tot_ref, w_ref, head_ref, mu_out_ref, coords_ref,
         a_ref, y_ref, acc_ref, cov_ref, soft_ref, dw_ref, z_ref) = refs
    else:
        (coords_ref, before_ref, infos_ref, turned_ref, hq_ref, mu_ref, lam_ref, wt_ref, ext_ref,
         load_ref, cover_ref, tot_ref, w_ref, head_ref,
         a_ref, y_ref, acc_ref, cov_ref, soft_ref, dw_ref, z_ref) = refs
    n = infos_ref.shape[2]
    nz, cols = lam_ref.shape
    width = coords_ref.shape[1]
    total = nz * cols
    tiles = total // BLOCK
    me_y, me_z, c = spots()
    w_ref[:, 0:width, :] = turned_ref[...]
    wt = wt_ref[...]
    lam = lam_ref[...]
    a1, a2, a3 = split3(64.0 * lam - hq_ref[...])
    one_c = jnp.ones((3, cols), F32)
    for r in range(nz):
        row = slice(r, r + 1)
        at = slice(r * cols, (r + 1) * cols)
        mw = jnp.broadcast_to(-64.0 * wt[row], (3, cols))
        aug = jnp.concatenate([a1[row].astype(F32), a2[row].astype(F32), a3[row].astype(F32), one_c, mw, jnp.zeros((7, cols), F32)], axis=0)
        w_ref[r, width:width + 16, :] = aug.astype(BF16)
        dw_ref[:, at] = jnp.broadcast_to(wt[row], (8, cols))
    w_ref[:, width + 16:, :] = jnp.zeros((nz, width - 16, cols), BF16)
    cov_ref[...] = jnp.zeros_like(cov_ref)
    soft_ref[...] = jnp.zeros_like(soft_ref)
    lane = lax.broadcasted_iota(jnp.int32, (ROWS, width), 1)
    pad = jnp.where(lane == 3, -30000.0, 0.0).astype(BF16)
    sel = (lax.broadcasted_iota(jnp.int32, (16, width), 0) == lax.broadcasted_iota(jnp.int32, (16, width), 1)).astype(F32).astype(BF16)
    offs = []
    off = jnp.int32(HEAD)
    one_r = jnp.ones((3, n), F32)
    if not first:
        a_ref[:, 0:width] = coords_ref[...]
        head_ref[:, 0:width] = before_ref[:, 0:width]
    for s in range(ny):
        valid = infos_ref[s, 0:1, :]
        if first:
            mu = infos_ref[s, 2:3, :] * valid
            mu_out_ref[s:s + 1, :] = mu
        else:
            mu = mu_ref[s:s + 1, :]
        b = jnp.where(valid > 0, infos_ref[s, 1:2, :], -30000.0)
        parts = [p.astype(F32) for p in split3(b) + split3(mu)]
        rows = jnp.concatenate([one_r] + parts + [jnp.zeros((7, n), F32)], axis=0).astype(BF16)
        side = tn(rows, sel).astype(BF16)
        count = jnp.sum(valid).astype(jnp.int32)
        off = pl.multiple_of(off, ALIGN)
        offs.append(off)
        if first:
            a_ref[pl.ds(off, n - HEAD), 0:width] = facs_ref[s, HEAD:]
            head_ref[s * HEAD:(s + 1) * HEAD, 0:width] = facs_ref[s, 0:HEAD]
        a_ref[pl.ds(off, n - HEAD), width:2 * width] = side[HEAD:]
        head_ref[s * HEAD:(s + 1) * HEAD, width:2 * width] = side[0:HEAD]
        off = off + ((jnp.maximum(count - HEAD, 0) + ALIGN - 1) // ALIGN) * ALIGN
    tail = pl.multiple_of(off, ALIGN)
    if first:
        a_ref[pl.ds(tail, ROWS), 0:width] = jnp.zeros((ROWS, width), BF16)
    a_ref[pl.ds(tail, ROWS), width:2 * width] = pad
    if first:
        coords_ref[...] = a_ref[:, 0:width]
    n_blocks = (off - HEAD + ROWS - 1) // ROWS
    scale = math.log2(math.e) / 6.4

    def dot(base, t, out):
        out[t] = jnp.dot(a_ref[pl.ds(base, ROWS), :], w_ref[t], preferred_element_type=F32)

    def phase(i, cur, nxt, opening=False):
        base = pl.multiple_of(HEAD + i * ROWS, ALIGN)
        for t in range(tiles):
            if opening and t + 1 < tiles:
                dot(HEAD, t + 1, cur)
            dot(pl.multiple_of(base + ROWS, ALIGN), t, nxt)
            spans = [slice(t * BLOCK + q * 128, t * BLOCK + (q + 1) * 128) for q in range(BLOCK // 128)]
            covs = [cov_ref[:, at] for at in spans]
            softs = [soft_ref[:, at] for at in spans]
            for r in range(0, ROWS, 32):
                slots = [pl.ds(pl.multiple_of(base + (r + 8 * s), 8), 8) for s in range(4)]
                loads = [acc_ref[at, :] for at in slots] if t else [jnp.zeros((8, 128), F32)] * 4
                for q in range(BLOCK // 128):
                    dw = dw_ref[:, spans[q]]
                    es = [jnp.exp2(cur[t, r + 8 * s:r + 8 * s + 8, q * 128:(q + 1) * 128] * scale) for s in range(4)]
                    us = [1.0 + e for e in es]
                    p01 = us[0] * us[1]
                    p23 = us[2] * us[3]
                    r01 = dw / p01
                    r23 = dw / p23
                    xs = [es[0] * (us[1] * r01), es[1] * (us[0] * r01), es[2] * (us[3] * r23), es[3] * (us[2] * r23)]
                    loads = [a + x for a, x in zip(loads, xs)]
                    covs[q] = covs[q] + ((xs[0] + xs[1]) + (xs[2] + xs[3]))
                    softs[q] = softs[q] + jnp.log(p01 * p23)
                for s in range(4):
                    acc_ref[slots[s], :] = loads[s]
            for q in range(BLOCK // 128):
                cov_ref[:, spans[q]] = covs[q]
                soft_ref[:, spans[q]] = softs[q]

    def body(i, _):
        phase(2 * i + 1, z_ref, y_ref)
        pl.when(2 * i + 2 < n_blocks)(lambda: phase(2 * i + 2, y_ref, z_ref))
        return 0

    dot(HEAD, 0, y_ref)
    phase(jnp.int32(0), y_ref, z_ref, True)
    lax.fori_loop(0, n_blocks // 2, body, 0)
    ones = jnp.ones((16, 128), BF16)
    for s in range(ny):
        for b in range(n // 128):
            at = pl.ds(pl.multiple_of(offs[s] + (b * 128 - HEAD), ALIGN), 128)
            own = (infos_ref[s, 0:1, b * 128:(b + 1) * 128] > 0) & (lax.broadcasted_iota(jnp.int32, (1, 128), 1) >= HEAD - b * 128)
            got = sum(nt(ones, p)[0:1] for p in split3(acc_ref[at, :])[:2])
            load_ref[s:s + 1, b * 128:(b + 1) * 128] = jnp.where(own, got, 0.0)
    soft = 0.0
    for r in range(nz):
        at = slice(r * cols, (r + 1) * cols)
        cover_ref[r:r + 1, :] = jnp.sum(cov_ref[:, at], axis=0, keepdims=True)
        soft = soft + soft_ref[:, at] * wt[r:r + 1]
    mu_all = mu_out_ref if first else mu_ref
    caps = infos_ref[me_y, 3:4, :]
    mine = jnp.sum(mu_all[pl.ds(me_y, 1), :] * caps)
    owned = jnp.sum(lam_ref[pl.ds(me_z, 1), :] * wt_ref[pl.ds(me_z, 1), :])
    here = owned - TAU * jnp.sum(soft) - jnp.where(c == 0, mine, 0.0)
    spot = lax.broadcasted_iota(jnp.int32, (1, 128), 1) == step
    tot_ref[...] = ext_ref[...] + jnp.where(spot, here, 0.0)


def head_rows(wt_ref, w_ref, head_ref, hy, hacc, hcov):
    tiles = w_ref.shape[0]
    scale = math.log2(math.e) / 6.4
    for t in range(tiles):
        hy[t] = jnp.dot(head_ref[...], w_ref[t], preferred_element_type=F32)
    hacc[...] = jnp.zeros_like(hacc)

    def body(t, soft):
        covs = [jnp.zeros((16, 128), F32)] * (BLOCK // 128)
        softs = [jnp.zeros((8, 128), F32)] * (BLOCK // 128)
        weights = wt_ref[pl.ds(t, 1), :]
        for r in range(0, head_ref.shape[0], 32):
            places = [slice(k // HEAD * 128 + k % HEAD, k // HEAD * 128 + k % HEAD + 16) for k in (r, r + 16)]
            loads = [hacc[at, :] for at in places]
            for q in range(BLOCK // 128):
                at = slice(q * 128, (q + 1) * 128)
                es = [jnp.exp2(hy[t, r + 16 * s:r + 16 * s + 16, at] * scale) for s in range(2)]
                us = [1.0 + e for e in es]
                p = us[0] * us[1]
                inv = weights[:, at] / p
                xs = [es[0] * (us[1] * inv), es[1] * (us[0] * inv)]
                loads = [a + x for a, x in zip(loads, xs)]
                covs[q] = covs[q] + (xs[0] + xs[1])
                softs[q] = softs[q] + jnp.log(p[0:8] * p[8:16])
            for at, load in zip(places, loads):
                hacc[at, :] = load
        hcov[pl.ds(t, 1), :] = jnp.concatenate([jnp.sum(v, axis=0, keepdims=True) for v in covs], axis=1)
        for q in range(BLOCK // 128):
            soft = soft + softs[q] * weights[:, q * 128:(q + 1) * 128]
        return soft

    return jnp.sum(lax.fori_loop(0, tiles, body, jnp.zeros((8, 128), F32)))


def far(n):
    return sorted(range(1, n), key=lambda d: -min(d, n - d))


def reduce_kernel(step, ny, nc, refs):
    last = step == ITERS - 1
    if last:
        (load_ref, cover_ref, lam_ref, wt_ref, mu_ref, infos_ref, tot_ref, w_ref, head_ref, open_ref, shut_ref,
         lam_out_ref, cap_out_ref, bound_ref, mu_out_ref, tot_out_ref, hy, hacc, hcov, hload,
         gotz, gotc, goty, mid, sz, rz, sc, rc, sy, ry, gott, gotp, midt, own, st, rt, sp, rp, sl, rl) = refs
    else:
        (load_ref, cover_ref, lam_ref, wt_ref, mu_ref, infos_ref, tot_ref, w_ref, head_ref,
         lam_out_ref, mu_out_ref, tot_out_ref, hy, hacc, hcov, hload,
         gotz, gotc, goty, mid, sz, rz, sc, rc, sy, ry) = refs
    size = 0.1 / (step + 1)
    y, z, c = spots()
    zp = [(y * NZ + lax.rem(z + d, NZ), c) for d in far(NZ)]
    yp = [(lax.rem(y + d, ny) * NZ + z, c) for d in far(ny)]
    cp = [(y * NZ + z, lax.rem(c + d, nc)) for d in far(nc)]
    plane = [(lax.rem(y + e, ny) * NZ + z, lax.rem(c + d, nc)) for e in far(ny) + [0] for d in far(nc) + [0] if e + d > 0]
    peers = zp + (plane if last else yp + cp)
    greet(peers)
    tot_out_ref[...] = tot_ref[...] - jnp.where(lax.broadcasted_iota(jnp.int32, (1, 128), 1) == step, TAU * head_rows(wt_ref, w_ref, head_ref, hy, hacc, hcov), 0.0)
    gotz[z] = (cover_ref[...] + hcov[...]) / wt_ref[...]
    ones = jnp.ones((16, 128), BF16)
    hload[...] = load_ref[...]
    for k in range(ny):
        part = split3(hacc[k * 128:(k + 1) * 128, :])[:2]
        hload[k:k + 1, 0:128] = load_ref[k:k + 1, 0:128] + sum(nt(ones, p)[0:1] for p in part)
    gotc[c] = hload[...]
    pl.semaphore_wait(pltpu.get_barrier_semaphore(), len(peers))
    if last:
        ts = [remote(tot_out_ref, gott.at[z], st.at[d], rt.at[d], peer) for d, peer in enumerate(zp)]
    zs = [remote(gotz.at[z], gotz.at[z], sz.at[d], rz.at[d], peer) for d, peer in enumerate(zp)]
    cs = [remote(gotc.at[c], gotc.at[c], sc.at[d], rc.at[d], peer) for d, peer in enumerate(cp)]
    for cpy in cs:
        cpy.wait_recv()
    total = gotc[0]
    for k in range(1, nc):
        total = total + gotc[k]
    mid[...] = total
    goty[y] = total
    ys = [remote(mid, goty.at[y], sy.at[d], ry.at[d], peer) for d, peer in enumerate(yp)]
    if last:
        gott[z] = tot_out_ref[...]
        for cpy in ts:
            cpy.wait_recv()
        total = gott[0]
        for k in range(1, NZ):
            total = total + gott[k]
        midt[...] = total
        gotp[y * nc + c] = total
        ps = [remote(midt, gotp.at[y * nc + c], sp.at[d], rp.at[d], peer) for d, peer in enumerate(plane)]
    for cpy in zs:
        cpy.wait_recv()
    cover = gotz[0]
    for k in range(1, NZ):
        cover = cover + gotz[k]
    lam = lam_ref[...] + size * wt_ref[...] * (1.0 - cover) / (1.0 + cover)
    if last:
        for r in range(NZ):
            own[r] = lam[r:r + 1]
            lam_out_ref[y * NZ + r] = lam[r:r + 1]
        ls = [remote(own, lam_out_ref.at[pl.ds(y * NZ, NZ)], sl.at[d], rl.at[d], peer) for d, peer in enumerate(yp)]
    else:
        lam_out_ref[...] = lam
    for cpy in ys:
        cpy.wait()
    load = goty[0]
    for k in range(1, ny):
        load = load + goty[k]
    for k in range(ny):
        row = slice(k, k + 1)
        valid = infos_ref[k, 0:1, :]
        cap = infos_ref[k, 3:4, :]
        got = load[row]
        mu = jnp.maximum(0.0, mu_ref[row, :] + size * (got - cap) / (got + jnp.where(valid > 0, cap, 1.0)))
        mu_out_ref[row, :] = mu * valid
    if last:
        n = open_ref.shape[1]
        parts = [v.astype(F32) for v in split3(mu_out_ref[pl.ds(y, 1), :])]
        rows = jnp.concatenate(parts + [jnp.zeros((13, n), F32)], axis=0).astype(BF16)
        got = jnp.dot(rows, onehot_of(open_ref[...]), preferred_element_type=F32)
        cap_out_ref[...] = jnp.where(open_ref[...] > 0, got[0:1] + got[1:2] + got[2:3], shut_ref[...])
        for cpy in ps:
            cpy.wait()
        total = gotp[0]
        for k in range(1, ny * nc):
            total = total + gotp[k]
        bound_ref[...] = total / (NZ * ny * nc * lam_ref.shape[1])
        for cpy in ls:
            cpy.wait()
        for cpy in ts:
            cpy.wait_send()
    for cpy in zs + cs:
        cpy.wait_send()


def finish_kernel(lam_ref, cap_ref, bound_ref, lam_out, cap_out, bound_out, sems):
    copies = [pltpu.make_async_copy(lam_ref, lam_out, sems.at[0]), pltpu.make_async_copy(cap_ref, cap_out, sems.at[1])]
    for cpy in copies:
        cpy.start()
    lane = lax.broadcasted_iota(jnp.int32, (1, 128), 1)
    for k in range(ITERS):
        bound_out[k] = jnp.sum(jnp.where(lane == k, bound_ref[...], 0.0))
    for cpy in copies:
        cpy.wait()


def params(cid=None, mib=24):
    return pltpu.CompilerParams(collective_id=cid, has_side_effects=True, vmem_limit_bytes=mib * 2 ** 20) if cid is not None else pltpu.CompilerParams(vmem_limit_bytes=mib * 2 ** 20)


def packed(kernel, *head):
    def run(*refs):
        kernel(*head, refs)
    return run


def work_of(ny, n, cols, width):
    scr = pltpu.VMEM
    rows = ny * n + 3 * ROWS
    total = NZ * cols
    return rows, [
        scr((rows, 2 * width), BF16),
        scr((total // BLOCK, ROWS, BLOCK), F32),
        scr((rows, 128), F32),
        scr((8, total), F32),
        scr((8, total), F32),
        scr((8, total), F32),
        scr((total // BLOCK, ROWS, BLOCK), F32),
    ]


def local(nf, nc, fac_coords, cust_coords, open_flags, demand, fixed_cost, capacity, cap_mult, cover_mult):
    n, width = fac_coords.shape
    cols = cust_coords.shape[0]
    ny = nf // NZ
    sd = jax.ShapeDtypeStruct
    dma = pltpu.SemaphoreType.DMA
    scr = pltpu.VMEM
    open_row = open_flags.reshape(1, n)
    hops = NZ // 2
    facs, infos, wt, lam, ext, shut, flags, turned, hq = pl.pallas_call(
        functools.partial(gather_kernel, ny),
        out_shape=(sd((ny, n, width), BF16), sd((ny, 8, n), F32),
                   sd((NZ, cols), F32), sd((NZ, cols), F32), sd((1, 128), F32), sd((1, n), F32), sd((1, n), jnp.int32),
                   sd((NZ, width, cols), BF16), sd((NZ, cols), F32)),
        in_specs=[HBM] * 8, out_specs=(VMEM,) * 9,
        scratch_shapes=[scr((NZ, cols, width), BF16), scr((1, n), jnp.int32), scr((n, width), BF16), scr((1, n), F32), scr((1, n), F32), scr((1, n), F32),
                        scr((1, NZ * cols), jnp.int32), scr((1, NZ * cols), F32),
                        dma((2, hops, CHUNKS)), dma((2, hops, CHUNKS)), dma((ny - 1, 2)), dma((ny - 1, 2)), dma((8,))],
        compiler_params=params(0), name="gather",
    )(*[pltpu.with_memory_space_constraint(v, pltpu.HBM) for v in (
        cust_coords, open_row, fac_coords, capacity.reshape(1, n), cap_mult.reshape(1, n), fixed_cost.reshape(1, n),
        demand.reshape(1, nf * cols), cover_mult.reshape(1, nf * cols))])
    rows, work = work_of(ny, n, cols, width)
    tot = ext
    mu = None
    for step in range(ITERS):
        last = step == ITERS - 1
        outs = (sd((ny, n), F32), sd((NZ, cols), F32), sd((1, 128), F32), sd((NZ, 2 * width, cols), BF16), sd((ny * HEAD, 2 * width), BF16))
        if step == 0:
            load, cover, tot, w, head, mu, coords = pl.pallas_call(
                packed(step_kernel, step, ny),
                out_shape=outs + (sd((ny, n), F32), sd((rows, width), BF16)),
                in_specs=[VMEM] * 7, out_specs=(VMEM,) * 7, scratch_shapes=work, compiler_params=params(), name="step",
            )(facs, infos, turned, hq, lam, wt, tot)
        else:
            load, cover, tot, w, head = pl.pallas_call(
                packed(step_kernel, step, ny),
                out_shape=outs, in_specs=[VMEM] * 9, out_specs=(VMEM,) * 5, scratch_shapes=work,
                compiler_params=params(), name="step",
            )(coords, head, infos, turned, hq, mu, lam, wt, tot)
        front = [scr((NZ, ny * HEAD, cols), F32), scr((ny * 128, 128), F32), scr((NZ, cols), F32), scr((ny, n), F32)]
        scratch = [scr((NZ, NZ, cols), F32), scr((nc, ny, n), F32), scr((ny, ny, n), F32), scr((ny, n), F32),
                   dma((NZ - 1,)), dma((NZ - 1,)), dma((nc - 1,)), dma((nc - 1,)), dma((ny - 1,)), dma((ny - 1,))]
        if not last:
            lam, mu, tot = pl.pallas_call(
                packed(reduce_kernel, step, ny, nc),
                out_shape=(sd((NZ, cols), F32), sd((ny, n), F32), sd((1, 128), F32)), in_specs=[VMEM] * 9, out_specs=(VMEM,) * 3,
                scratch_shapes=front + scratch, compiler_params=params(1 + step), name="reduce",
            )(load, cover, lam, wt, mu, infos, tot, w, head)
        else:
            plane = ny * nc
            lam_all, cap_final, bounds = pl.pallas_call(
                packed(reduce_kernel, step, ny, nc),
                out_shape=(sd((nf, 1, cols), F32), sd((1, n), F32), sd((1, 128), F32)), in_specs=[VMEM] * 11, out_specs=(VMEM,) * 3,
                scratch_shapes=[scr((ny, n), F32), scr((1, 128), F32)] + front + scratch + [
                    scr((NZ, 1, 128), F32), scr((plane, 1, 128), F32), scr((1, 128), F32), scr((NZ, 1, cols), F32),
                    dma((NZ - 1,)), dma((NZ - 1,)), dma((plane - 1,)), dma((plane - 1,)), dma((ny - 1,)), dma((ny - 1,))],
                compiler_params=params(1 + step), name="reduce",
            )(load, cover, lam, wt, mu, infos, tot, w, head, flags, shut)
    lam_all, cap_final, bounds = pl.pallas_call(
        finish_kernel, out_shape=(sd((nf, 1, cols), F32), sd((1, n), F32), sd((ITERS,), F32)),
        in_specs=[VMEM] * 3, out_specs=(HBM, HBM, pl.BlockSpec(memory_space=pltpu.SMEM)), scratch_shapes=[dma((2,))],
        compiler_params=params(), name="finish",
    )(lam_all, cap_final, bounds)
    return lam_all.reshape(nf * cols), cap_final.reshape(n), bounds


def solution(mesh):
    nf, nc = mesh.shape["fac"], mesh.shape["cust"]
    return jax.shard_map(
        functools.partial(local, nf, nc),
        mesh=mesh,
        in_specs=(P("fac", None), P(("cust", "fac"), None), P("fac"), P("cust"), P("fac"), P("fac"), P("fac"), P("cust")),
        out_specs=(P("cust"), P("fac"), P()),
        check_vma=False,
    )
```

```python
import functools
import math

import jax
import jax.numpy as jnp
from jax import lax
from jax.experimental import pallas as pl
from jax.experimental.pallas import tpu as pltpu
from jax.sharding import PartitionSpec as P

MESH = pl.DeviceIdType.MESH
ITERS = 3
TAU = 0.1
ALIGN = 16
ROWS = 160
HEAD = 80
BLOCK = 512
CHUNKS = 16
NZ = 8
F32 = jnp.float32
BF16 = jnp.bfloat16
VMEM = pl.BlockSpec(memory_space=pltpu.VMEM)
HBM = pl.BlockSpec(memory_space=pltpu.HBM)


def split3(v):
    a = v.astype(BF16)
    r = v - a.astype(F32)
    b = r.astype(BF16)
    c = (r - b.astype(F32)).astype(BF16)
    return a, b, c


def onehot_of(open_row):
    n = open_row.shape[1]
    flags = jnp.broadcast_to(open_row.astype(F32), (16, n)).astype(BF16)
    tri = (lax.broadcasted_iota(jnp.int32, (n, n), 0) <= lax.broadcasted_iota(jnp.int32, (n, n), 1)).astype(F32).astype(BF16)
    pos = jnp.dot(flags, tri, preferred_element_type=F32)[0:1]
    pos = jnp.where(open_row > 0, pos - 1.0, -1.0).astype(jnp.int32)
    hit = lax.broadcasted_iota(jnp.int32, (n, n), 0) == pos
    return jnp.where(hit, 1.0, 0.0).astype(BF16)


def nt(a, b):
    return lax.dot_general(a, b, (((1,), (1,)), ((), ())), preferred_element_type=F32)


def tn(a, b):
    return lax.dot_general(a, b, (((0,), (0,)), ((), ())), preferred_element_type=F32)


def spots():
    f, c = lax.axis_index("fac"), lax.axis_index("cust")
    return f // NZ, lax.rem(f, NZ), c


def greet(peers):
    barrier = pltpu.get_barrier_semaphore()
    for peer in peers:
        pl.semaphore_signal(barrier, inc=1, device_id=peer, device_id_type=MESH)


def sync(peers):
    greet(peers)
    pl.semaphore_wait(pltpu.get_barrier_semaphore(), len(peers))


def remote(src, dst, send, recv, peer):
    cpy = pltpu.make_async_remote_copy(src, dst, send, recv, device_id=peer, device_id_type=MESH)
    cpy.start()
    return cpy


def compact(opened, fac, mu, cap):
    n, width = fac.shape
    hot = onehot_of(opened)
    comp = jnp.dot(hot, fac, preferred_element_type=F32).astype(BF16)
    sq = fac.astype(F32) ** 2
    s1, s2, _ = split3(sq)
    ones = jnp.ones((16, width), BF16)
    half = -0.5 * (nt(ones, s1) + nt(ones, s2))[0:1]
    rows = [jnp.ones((1, n), BF16)]
    for v in (half, mu, cap):
        rows.extend(split3(v))
    rows = [r.astype(F32) for r in rows] + [jnp.zeros((6, n), F32)]
    got = nt(jnp.concatenate(rows, axis=0).astype(BF16), hot)
    rows = [got[0:1]] + [got[3 * m + 1:3 * m + 2] + got[3 * m + 2:3 * m + 3] + got[3 * m + 3:3 * m + 4] for m in range(3)]
    return comp, jnp.concatenate(rows + [jnp.zeros((4, n), F32)], axis=0)


def gather_kernel(ny, cust_hbm, open_hbm, fac_hbm, cap_hbm, mu_hbm, fixed_hbm, demand_hbm, cover_hbm,
                  facs_ref, infos_ref, wt_ref, lam_ref, ext_ref, shut_ref, flags_ref, turned_ref, hq_ref,
                  all_ref, open_ref, fac_ref, cap_ref, mu_ref, fixed_ref, demand_ref, cover_ref, sz, rz, sy, ry, loc):
    y, z, c = spots()
    nz, cols = wt_ref.shape
    hops = NZ // 2
    zp = [(y * NZ + lax.rem(z + s, NZ), c) for s in (1, NZ - 1)]
    yp = [(lax.rem(y + d, ny) * NZ + z, c) for d in range(1, ny)]
    part = cols // CHUNKS
    segment = pl.ds(pl.multiple_of(y * (nz * cols), nz * cols), nz * cols)
    pairs = [(cust_hbm, all_ref.at[z]), (fac_hbm, fac_ref), (open_hbm, open_ref), (cap_hbm, cap_ref), (mu_hbm, mu_ref),
             (fixed_hbm, fixed_ref), (demand_hbm.at[:, segment], demand_ref), (cover_hbm.at[:, segment], cover_ref)]
    own = [pltpu.make_async_copy(a, b, loc.at[k]) for k, (a, b) in enumerate(pairs)]
    for cpy in own:
        cpy.start()
    sync(zp + yp)

    def move(d, s, j):
        src = lax.rem(z + (NZ - s if d == 0 else s), NZ)
        at = pl.ds(j * part, part)
        return remote(all_ref.at[src, at], all_ref.at[src, at], sz.at[d, s, j], rz.at[d, s, j], zp[d])

    def valid(d, s, j):
        return s < hops - 1 or (s == hops - 1 and (j < CHUNKS // 2) == (d == 0))

    ring = {}
    own[0].wait()
    for j in range(CHUNKS):
        for d in range(2):
            if valid(d, 0, j):
                ring[d, 0, j] = move(d, 0, j)
    for cpy in own[1:]:
        cpy.wait()
    comp, info = compact(open_ref[...], fac_ref[...], mu_ref[...], cap_ref[...])
    facs_ref[y] = comp
    infos_ref[y] = info
    for r in range(nz):
        mine = slice(r * cols, (r + 1) * cols)
        wt_ref[r:r + 1, :] = demand_ref[:, mine].astype(F32)
        lam_ref[r:r + 1, :] = cover_ref[:, mine]
    opened = open_ref[...].astype(F32)
    shut = mu_ref[...]
    ext = jnp.zeros((1, 128), F32)
    lane = lax.broadcasted_iota(jnp.int32, (1, 128), 1)
    for k in range(ITERS):
        fixed = jnp.sum(opened * fixed_ref[...] - (1.0 - opened) * shut * cap_ref[...])
        ext = ext + jnp.where((lane == k) & (c == 0), fixed, 0.0)
        shut = jnp.maximum(0.0, shut - 0.1 / (k + 1))
    ext_ref[...] = ext
    shut_ref[...] = shut
    flags_ref[...] = open_ref[...]
    side = []
    for k, peer in enumerate(yp):
        side.append(remote(infos_ref.at[y], infos_ref.at[y], sy.at[k, 0], ry.at[k, 0], peer))
        side.append(remote(facs_ref.at[y], facs_ref.at[y], sy.at[k, 1], ry.at[k, 1], peer))
    width = fac_ref.shape[1]
    eye = (lax.broadcasted_iota(jnp.int32, (width, width), 0) == lax.broadcasted_iota(jnp.int32, (width, width), 1)).astype(F32).astype(BF16)

    def turn(k):
        turned = nt(eye, all_ref[k])
        turned_ref[k] = turned.astype(BF16)
        hq_ref[pl.ds(k, 1), :] = 0.5 * jnp.sum(turned * turned, axis=0, keepdims=True)

    turn(z)
    for s in range(hops):
        for j in range(CHUNKS):
            for d in range(2):
                if valid(d, s, j):
                    ring[d, s, j].wait_recv()
                    if valid(d, s + 1, j):
                        ring[d, s + 1, j] = move(d, s + 1, j)
        turn(lax.rem(z + s + 1, NZ))
        if s < hops - 1:
            turn(lax.rem(z + NZ - s - 1, NZ))
    for cpy in ring.values():
        cpy.wait_send()
    for cpy in side:
        cpy.wait()


def step_kernel(step, ny, refs):
    first = step == 0
    if first:
        (facs_ref, infos_ref, turned_ref, hq_ref, lam_ref, wt_ref, ext_ref,
         load_ref, cover_ref, tot_ref, w_ref, head_ref, mu_out_ref, coords_ref,
         a_ref, y_ref, acc_ref, cov_ref, soft_ref, dw_ref, z_ref) = refs
    else:
        (coords_ref, before_ref, infos_ref, turned_ref, hq_ref, mu_ref, lam_ref, wt_ref, ext_ref,
         load_ref, cover_ref, tot_ref, w_ref, head_ref,
         a_ref, y_ref, acc_ref, cov_ref, soft_ref, dw_ref, z_ref) = refs
    n = infos_ref.shape[2]
    nz, cols = lam_ref.shape
    width = coords_ref.shape[1]
    total = nz * cols
    tiles = total // BLOCK
    me_y, me_z, c = spots()
    w_ref[:, 0:width, :] = turned_ref[...]
    wt = wt_ref[...]
    lam = lam_ref[...]
    a1, a2, a3 = split3(64.0 * lam - hq_ref[...])
    one_c = jnp.ones((3, cols), F32)
    for r in range(nz):
        row = slice(r, r + 1)
        at = slice(r * cols, (r + 1) * cols)
        mw = jnp.broadcast_to(-64.0 * wt[row], (3, cols))
        aug = jnp.concatenate([a1[row].astype(F32), a2[row].astype(F32), a3[row].astype(F32), one_c, mw, jnp.zeros((7, cols), F32)], axis=0)
        w_ref[r, width:width + 16, :] = aug.astype(BF16)
        dw_ref[:, at] = jnp.broadcast_to(wt[row], (8, cols))
    w_ref[:, width + 16:, :] = jnp.zeros((nz, width - 16, cols), BF16)
    cov_ref[...] = jnp.zeros_like(cov_ref)
    soft_ref[...] = jnp.zeros_like(soft_ref)
    lane = lax.broadcasted_iota(jnp.int32, (ROWS, width), 1)
    pad = jnp.where(lane == 3, -30000.0, 0.0).astype(BF16)
    sel = (lax.broadcasted_iota(jnp.int32, (16, width), 0) == lax.broadcasted_iota(jnp.int32, (16, width), 1)).astype(F32).astype(BF16)
    offs = []
    off = jnp.int32(HEAD)
    one_r = jnp.ones((3, n), F32)
    if not first:
        a_ref[:, 0:width] = coords_ref[...]
        head_ref[:, 0:width] = before_ref[:, 0:width]
    for s in range(ny):
        valid = infos_ref[s, 0:1, :]
        if first:
            mu = infos_ref[s, 2:3, :] * valid
            mu_out_ref[s:s + 1, :] = mu
        else:
            mu = mu_ref[s:s + 1, :]
        b = jnp.where(valid > 0, infos_ref[s, 1:2, :], -30000.0)
        parts = [p.astype(F32) for p in split3(b) + split3(mu)]
        rows = jnp.concatenate([one_r] + parts + [jnp.zeros((7, n), F32)], axis=0).astype(BF16)
        side = tn(rows, sel).astype(BF16)
        count = jnp.sum(valid).astype(jnp.int32)
        off = pl.multiple_of(off, ALIGN)
        offs.append(off)
        if first:
            a_ref[pl.ds(off, n - HEAD), 0:width] = facs_ref[s, HEAD:]
            head_ref[s * HEAD:(s + 1) * HEAD, 0:width] = facs_ref[s, 0:HEAD]
        a_ref[pl.ds(off, n - HEAD), width:2 * width] = side[HEAD:]
        head_ref[s * HEAD:(s + 1) * HEAD, width:2 * width] = side[0:HEAD]
        off = off + ((jnp.maximum(count - HEAD, 0) + ALIGN - 1) // ALIGN) * ALIGN
    tail = pl.multiple_of(off, ALIGN)
    if first:
        a_ref[pl.ds(tail, ROWS), 0:width] = jnp.zeros((ROWS, width), BF16)
    a_ref[pl.ds(tail, ROWS), width:2 * width] = pad
    if first:
        coords_ref[...] = a_ref[:, 0:width]
    n_blocks = (off - HEAD + ROWS - 1) // ROWS
    scale = math.log2(math.e) / 6.4

    def dot(base, t, out):
        out[t] = jnp.dot(a_ref[pl.ds(base, ROWS), :], w_ref[t], preferred_element_type=F32)

    def phase(i, cur, nxt, opening=False):
        base = pl.multiple_of(HEAD + i * ROWS, ALIGN)
        for t in range(tiles):
            if opening and t + 1 < tiles:
                dot(HEAD, t + 1, cur)
            dot(pl.multiple_of(base + ROWS, ALIGN), t, nxt)
            spans = [slice(t * BLOCK + q * 128, t * BLOCK + (q + 1) * 128) for q in range(BLOCK // 128)]
            covs = [cov_ref[:, at] for at in spans]
            softs = [soft_ref[:, at] for at in spans]
            for r in range(0, ROWS, 32):
                slots = [pl.ds(pl.multiple_of(base + (r + 8 * s), 8), 8) for s in range(4)]
                loads = [acc_ref[at, :] for at in slots] if t else [jnp.zeros((8, 128), F32)] * 4
                for q in range(BLOCK // 128):
                    dw = dw_ref[:, spans[q]]
                    es = [jnp.exp2(cur[t, r + 8 * s:r + 8 * s + 8, q * 128:(q + 1) * 128] * scale) for s in range(4)]
                    us = [1.0 + e for e in es]
                    p01 = us[0] * us[1]
                    p23 = us[2] * us[3]
                    r01 = dw / p01
                    r23 = dw / p23
                    xs = [es[0] * (us[1] * r01), es[1] * (us[0] * r01), es[2] * (us[3] * r23), es[3] * (us[2] * r23)]
                    loads = [a + x for a, x in zip(loads, xs)]
                    covs[q] = covs[q] + ((xs[0] + xs[1]) + (xs[2] + xs[3]))
                    softs[q] = softs[q] + jnp.log(p01 * p23)
                for s in range(4):
                    acc_ref[slots[s], :] = loads[s]
            for q in range(BLOCK // 128):
                cov_ref[:, spans[q]] = covs[q]
                soft_ref[:, spans[q]] = softs[q]

    def body(i, _):
        phase(2 * i + 1, z_ref, y_ref)
        pl.when(2 * i + 2 < n_blocks)(lambda: phase(2 * i + 2, y_ref, z_ref))
        return 0

    dot(HEAD, 0, y_ref)
    phase(jnp.int32(0), y_ref, z_ref, True)
    lax.fori_loop(0, n_blocks // 2, body, 0)
    ones = jnp.ones((16, 128), BF16)
    for s in range(ny):
        for b in range(n // 128):
            at = pl.ds(pl.multiple_of(offs[s] + (b * 128 - HEAD), ALIGN), 128)
            own = (infos_ref[s, 0:1, b * 128:(b + 1) * 128] > 0) & (lax.broadcasted_iota(jnp.int32, (1, 128), 1) >= HEAD - b * 128)
            got = sum(nt(ones, p)[0:1] for p in split3(acc_ref[at, :])[:2])
            load_ref[s:s + 1, b * 128:(b + 1) * 128] = jnp.where(own, got, 0.0)
    soft = 0.0
    for r in range(nz):
        at = slice(r * cols, (r + 1) * cols)
        cover_ref[r:r + 1, :] = jnp.sum(cov_ref[:, at], axis=0, keepdims=True)
        soft = soft + soft_ref[:, at] * wt[r:r + 1]
    mu_all = mu_out_ref if first else mu_ref
    caps = infos_ref[me_y, 3:4, :]
    mine = jnp.sum(mu_all[pl.ds(me_y, 1), :] * caps)
    owned = jnp.sum(lam_ref[pl.ds(me_z, 1), :] * wt_ref[pl.ds(me_z, 1), :])
    here = owned - TAU * jnp.sum(soft) - jnp.where(c == 0, mine, 0.0)
    spot = lax.broadcasted_iota(jnp.int32, (1, 128), 1) == step
    tot_ref[...] = ext_ref[...] + jnp.where(spot, here, 0.0)


def head_rows(wt_ref, w_ref, head_ref, hy, hacc, hcov):
    tiles = w_ref.shape[0]
    scale = math.log2(math.e) / 6.4
    for t in range(tiles):
        hy[t] = jnp.dot(head_ref[...], w_ref[t], preferred_element_type=F32)
    hacc[...] = jnp.zeros_like(hacc)

    def body(t, soft):
        covs = [jnp.zeros((16, 128), F32)] * (BLOCK // 128)
        softs = [jnp.zeros((8, 128), F32)] * (BLOCK // 128)
        weights = wt_ref[pl.ds(t, 1), :]
        for r in range(0, head_ref.shape[0], 32):
            places = [slice(k // HEAD * 128 + k % HEAD, k // HEAD * 128 + k % HEAD + 16) for k in (r, r + 16)]
            loads = [hacc[at, :] for at in places]
            for q in range(BLOCK // 128):
                at = slice(q * 128, (q + 1) * 128)
                es = [jnp.exp2(hy[t, r + 16 * s:r + 16 * s + 16, at] * scale) for s in range(2)]
                us = [1.0 + e for e in es]
                p = us[0] * us[1]
                inv = weights[:, at] / p
                xs = [es[0] * (us[1] * inv), es[1] * (us[0] * inv)]
                loads = [a + x for a, x in zip(loads, xs)]
                covs[q] = covs[q] + (xs[0] + xs[1])
                softs[q] = softs[q] + jnp.log(p[0:8] * p[8:16])
            for at, load in zip(places, loads):
                hacc[at, :] = load
        hcov[pl.ds(t, 1), :] = jnp.concatenate([jnp.sum(v, axis=0, keepdims=True) for v in covs], axis=1)
        for q in range(BLOCK // 128):
            soft = soft + softs[q] * weights[:, q * 128:(q + 1) * 128]
        return soft

    return jnp.sum(lax.fori_loop(0, tiles, body, jnp.zeros((8, 128), F32)))


def far(n):
    return sorted(range(1, n), key=lambda d: -min(d, n - d))


def reduce_kernel(step, ny, nc, refs):
    last = step == ITERS - 1
    if last:
        (load_ref, cover_ref, lam_ref, wt_ref, mu_ref, infos_ref, tot_ref, w_ref, head_ref, open_ref, shut_ref,
         lam_out_ref, cap_out_ref, bound_ref, mu_out_ref, tot_out_ref, hy, hacc, hcov, hload,
         gotz, gotc, goty, mid, sz, rz, sc, rc, sy, ry, gott, gotp, midt, own, st, rt, sp, rp, sl, rl) = refs
    else:
        (load_ref, cover_ref, lam_ref, wt_ref, mu_ref, infos_ref, tot_ref, w_ref, head_ref,
         lam_out_ref, mu_out_ref, tot_out_ref, hy, hacc, hcov, hload,
         gotz, gotc, goty, mid, sz, rz, sc, rc, sy, ry) = refs
    size = 0.1 / (step + 1)
    y, z, c = spots()
    zp = [(y * NZ + lax.rem(z + d, NZ), c) for d in far(NZ)]
    yp = [(lax.rem(y + d, ny) * NZ + z, c) for d in far(ny)]
    cp = [(y * NZ + z, lax.rem(c + d, nc)) for d in far(nc)]
    plane = [(lax.rem(y + e, ny) * NZ + z, lax.rem(c + d, nc)) for e in far(ny) + [0] for d in far(nc) + [0] if e + d > 0]
    peers = zp + (plane if last else yp + cp)
    greet(peers)
    tot_out_ref[...] = tot_ref[...] - jnp.where(lax.broadcasted_iota(jnp.int32, (1, 128), 1) == step, TAU * head_rows(wt_ref, w_ref, head_ref, hy, hacc, hcov), 0.0)
    gotz[z] = (cover_ref[...] + hcov[...]) / wt_ref[...]
    ones = jnp.ones((16, 128), BF16)
    hload[...] = load_ref[...]
    for k in range(ny):
        part = split3(hacc[k * 128:(k + 1) * 128, :])[:2]
        hload[k:k + 1, 0:128] = load_ref[k:k + 1, 0:128] + sum(nt(ones, p)[0:1] for p in part)
    gotc[c] = hload[...]
    pl.semaphore_wait(pltpu.get_barrier_semaphore(), len(peers))
    if last:
        ts = [remote(tot_out_ref, gott.at[z], st.at[d], rt.at[d], peer) for d, peer in enumerate(zp)]
    zs = [remote(gotz.at[z], gotz.at[z], sz.at[d], rz.at[d], peer) for d, peer in enumerate(zp)]
    cs = [remote(gotc.at[c], gotc.at[c], sc.at[d], rc.at[d], peer) for d, peer in enumerate(cp)]
    for cpy in cs:
        cpy.wait_recv()
    total = gotc[0]
    for k in range(1, nc):
        total = total + gotc[k]
    mid[...] = total
    goty[y] = total
    ys = [remote(mid, goty.at[y], sy.at[d], ry.at[d], peer) for d, peer in enumerate(yp)]
    if last:
        gott[z] = tot_out_ref[...]
        for cpy in ts:
            cpy.wait_recv()
        total = gott[0]
        for k in range(1, NZ):
            total = total + gott[k]
        midt[...] = total
        gotp[y * nc + c] = total
        ps = [remote(midt, gotp.at[y * nc + c], sp.at[d], rp.at[d], peer) for d, peer in enumerate(plane)]
    for cpy in zs:
        cpy.wait_recv()
    cover = gotz[0]
    for k in range(1, NZ):
        cover = cover + gotz[k]
    lam = lam_ref[...] + size * wt_ref[...] * (1.0 - cover) / (1.0 + cover)
    if last:
        for r in range(NZ):
            own[r] = lam[r:r + 1]
            lam_out_ref[y * NZ + r] = lam[r:r + 1]
        ls = [remote(own, lam_out_ref.at[pl.ds(y * NZ, NZ)], sl.at[d], rl.at[d], peer) for d, peer in enumerate(yp)]
    else:
        lam_out_ref[...] = lam
    for cpy in ys:
        cpy.wait()
    load = goty[0]
    for k in range(1, ny):
        load = load + goty[k]
    for k in range(ny):
        row = slice(k, k + 1)
        valid = infos_ref[k, 0:1, :]
        cap = infos_ref[k, 3:4, :]
        got = load[row]
        mu = jnp.maximum(0.0, mu_ref[row, :] + size * (got - cap) / (got + jnp.where(valid > 0, cap, 1.0)))
        mu_out_ref[row, :] = mu * valid
    if last:
        n = open_ref.shape[1]
        parts = [v.astype(F32) for v in split3(mu_out_ref[pl.ds(y, 1), :])]
        rows = jnp.concatenate(parts + [jnp.zeros((13, n), F32)], axis=0).astype(BF16)
        got = jnp.dot(rows, onehot_of(open_ref[...]), preferred_element_type=F32)
        cap_out_ref[...] = jnp.where(open_ref[...] > 0, got[0:1] + got[1:2] + got[2:3], shut_ref[...])
        for cpy in ps:
            cpy.wait()
        total = gotp[0]
        for k in range(1, ny * nc):
            total = total + gotp[k]
        bound_ref[...] = total / (NZ * ny * nc * lam_ref.shape[1])
        for cpy in ls:
            cpy.wait()
        for cpy in ts:
            cpy.wait_send()
    for cpy in zs + cs:
        cpy.wait_send()


def finish_kernel(lam_ref, cap_ref, bound_ref, lam_out, cap_out, bound_out, sems):
    copies = [pltpu.make_async_copy(lam_ref, lam_out, sems.at[0]), pltpu.make_async_copy(cap_ref, cap_out, sems.at[1])]
    for cpy in copies:
        cpy.start()
    lane = lax.broadcasted_iota(jnp.int32, (1, 128), 1)
    for k in range(ITERS):
        bound_out[k] = jnp.sum(jnp.where(lane == k, bound_ref[...], 0.0))
    for cpy in copies:
        cpy.wait()


def params(cid=None, mib=24):
    return pltpu.CompilerParams(collective_id=cid, has_side_effects=True, vmem_limit_bytes=mib * 2 ** 20) if cid is not None else pltpu.CompilerParams(vmem_limit_bytes=mib * 2 ** 20)


def packed(kernel, *head):
    def run(*refs):
        kernel(*head, refs)
    return run


def work_of(ny, n, cols, width):
    scr = pltpu.VMEM
    rows = ny * n + 3 * ROWS
    total = NZ * cols
    return rows, [
        scr((rows, 2 * width), BF16),
        scr((total // BLOCK, ROWS, BLOCK), F32),
        scr((rows, 128), F32),
        scr((8, total), F32),
        scr((8, total), F32),
        scr((8, total), F32),
        scr((total // BLOCK, ROWS, BLOCK), F32),
    ]


def local(nf, nc, fac_coords, cust_coords, open_flags, demand, fixed_cost, capacity, cap_mult, cover_mult):
    n, width = fac_coords.shape
    cols = cust_coords.shape[0]
    ny = nf // NZ
    sd = jax.ShapeDtypeStruct
    dma = pltpu.SemaphoreType.DMA
    scr = pltpu.VMEM
    open_row = open_flags.reshape(1, n)
    hops = NZ // 2
    facs, infos, wt, lam, ext, shut, flags, turned, hq = pl.pallas_call(
        functools.partial(gather_kernel, ny),
        out_shape=(sd((ny, n, width), BF16), sd((ny, 8, n), F32),
                   sd((NZ, cols), F32), sd((NZ, cols), F32), sd((1, 128), F32), sd((1, n), F32), sd((1, n), jnp.int32),
                   sd((NZ, width, cols), BF16), sd((NZ, cols), F32)),
        in_specs=[HBM] * 8, out_specs=(VMEM,) * 9,
        scratch_shapes=[scr((NZ, cols, width), BF16), scr((1, n), jnp.int32), scr((n, width), BF16), scr((1, n), F32), scr((1, n), F32), scr((1, n), F32),
                        scr((1, NZ * cols), jnp.int32), scr((1, NZ * cols), F32),
                        dma((2, hops, CHUNKS)), dma((2, hops, CHUNKS)), dma((ny - 1, 2)), dma((ny - 1, 2)), dma((8,))],
        compiler_params=params(0), name="gather",
    )(*[pltpu.with_memory_space_constraint(v, pltpu.HBM) for v in (
        cust_coords, open_row, fac_coords, capacity.reshape(1, n), cap_mult.reshape(1, n), fixed_cost.reshape(1, n),
        demand.reshape(1, nf * cols), cover_mult.reshape(1, nf * cols))])
    rows, work = work_of(ny, n, cols, width)
    tot = ext
    mu = None
    for step in range(ITERS):
        last = step == ITERS - 1
        outs = (sd((ny, n), F32), sd((NZ, cols), F32), sd((1, 128), F32), sd((NZ, 2 * width, cols), BF16), sd((ny * HEAD, 2 * width), BF16))
        if step == 0:
            load, cover, tot, w, head, mu, coords = pl.pallas_call(
                packed(step_kernel, step, ny),
                out_shape=outs + (sd((ny, n), F32), sd((rows, width), BF16)),
                in_specs=[VMEM] * 7, out_specs=(VMEM,) * 7, scratch_shapes=work, compiler_params=params(), name="step",
            )(facs, infos, turned, hq, lam, wt, tot)
        else:
            load, cover, tot, w, head = pl.pallas_call(
                packed(step_kernel, step, ny),
                out_shape=outs, in_specs=[VMEM] * 9, out_specs=(VMEM,) * 5, scratch_shapes=work,
                compiler_params=params(), name="step",
            )(coords, head, infos, turned, hq, mu, lam, wt, tot)
        front = [scr((NZ, ny * HEAD, cols), F32), scr((ny * 128, 128), F32), scr((NZ, cols), F32), scr((ny, n), F32)]
        scratch = [scr((NZ, NZ, cols), F32), scr((nc, ny, n), F32), scr((ny, ny, n), F32), scr((ny, n), F32),
                   dma((NZ - 1,)), dma((NZ - 1,)), dma((nc - 1,)), dma((nc - 1,)), dma((ny - 1,)), dma((ny - 1,))]
        if not last:
            lam, mu, tot = pl.pallas_call(
                packed(reduce_kernel, step, ny, nc),
                out_shape=(sd((NZ, cols), F32), sd((ny, n), F32), sd((1, 128), F32)), in_specs=[VMEM] * 9, out_specs=(VMEM,) * 3,
                scratch_shapes=front + scratch, compiler_params=params(1 + step), name="reduce",
            )(load, cover, lam, wt, mu, infos, tot, w, head)
        else:
            plane = ny * nc
            lam_all, cap_final, bounds = pl.pallas_call(
                packed(reduce_kernel, step, ny, nc),
                out_shape=(sd((nf, 1, cols), F32), sd((1, n), F32), sd((1, 128), F32)), in_specs=[VMEM] * 11, out_specs=(VMEM,) * 3,
                scratch_shapes=[scr((ny, n), F32), scr((1, 128), F32)] + front + scratch + [
                    scr((NZ, 1, 128), F32), scr((plane, 1, 128), F32), scr((1, 128), F32), scr((NZ, 1, cols), F32),
                    dma((NZ - 1,)), dma((NZ - 1,)), dma((plane - 1,)), dma((plane - 1,)), dma((ny - 1,)), dma((ny - 1,))],
                compiler_params=params(1 + step), name="reduce",
            )(load, cover, lam, wt, mu, infos, tot, w, head, flags, shut)
    lam_all, cap_final, bounds = pl.pallas_call(
        finish_kernel, out_shape=(sd((nf, 1, cols), F32), sd((1, n), F32), sd((ITERS,), F32)),
        in_specs=[VMEM] * 3, out_specs=(HBM, HBM, pl.BlockSpec(memory_space=pltpu.SMEM)), scratch_shapes=[dma((2,))],
        compiler_params=params(), name="finish",
    )(lam_all, cap_final, bounds)
    return lam_all.reshape(nf * cols), cap_final.reshape(n), bounds


def solution(mesh):
    nf, nc = mesh.shape["fac"], mesh.shape["cust"]
    return jax.shard_map(
        functools.partial(local, nf, nc),
        mesh=mesh,
        in_specs=(P("fac", None), P(("cust", "fac"), None), P("fac"), P("cust"), P("fac"), P("fac"), P("fac"), P("cust")),
        out_specs=(P("cust"), P("fac"), P()),
        check_vma=False,
    )
```
